256 devices in a mesh: row: 16 (over z, core), col: 16 (over y, x).
Axes of the slice: x: 4, y: 4, z: 8, core: 2. Of those that a mesh axis runs over, the one named last changes fastest.
Arguments:
- y_panels: bfloat16 [2, 1024, 4096], P(None, 'row', 'col'), may hold values from -6 to 6
- tri_inverse: bfloat16 [2, 1024, 1024], P(None, 'row', 'col'), may hold values from -1.5 to 1.5, as said below
- coupling: bfloat16 [1024, 1024], P('row', 'col'), may hold values from -0.1875 to 0.1875
- rest_factor: bfloat16 [40960, 2, 1024], P('row'), may hold values from -0.03125 to 0.03125
- rest_coeffs: bfloat16 [40960, 4096], P('row', 'col'), may hold values from -6 to 6
- occupations: float32 [4096], P('col'), may hold values from 0.02 to 1
Outputs:
- panel_coeffs: bfloat16 [2, 1024, 4096], P(None, 'row', 'col')
- density: bfloat16 [40960, 512], P(('row', 'col'))
The draws below stay inside these ranges and needn't reach their ends.
Inputs may be any that keep to these rules, and one draw needn't show every extreme that they name: `tri_inverse`: each block is upper triangular with diagonal entries between 0.6 and 1.4.
All inputs are finite; a program needn't handle non-finite values.
Results may differ from the reference program's by a relative error of at most 0.025.
Values may be sent and summed in bfloat16 or wider, within the bound.
A program may use at most 128 MiB of HBM per device.

```python
import math
import jax
import jax.numpy as jnp
from jax import lax

STATES = 4096
PANEL = 1024
STRIP = 512
REST = 40960


def draw_tri_inverse(key, part):
    upper_key = jax.random.fold_in(key, 11)
    diagonal_key = jax.random.fold_in(key, 12)
    upper = jax.random.normal(upper_key, (2, PANEL, PANEL), jnp.float32) * (0.6 / PANEL ** 0.5)
    diagonal = jax.random.uniform(diagonal_key, (2, PANEL), jnp.float32, 0.6, 1.4)
    row_index = jnp.arange(PANEL)[:, None]
    column_index = jnp.arange(PANEL)[None, :]
    triangle = (column_index > row_index)[None, :, :]
    identity = (column_index == row_index)[None, :, :]
    upper = jnp.clip(upper, -1.0, 1.0)
    blocks = jnp.where(triangle, upper, 0.0) + jnp.where(identity, diagonal[:, :, None], 0.0)
    return blocks.astype(jnp.bfloat16)


def levels(rng, dims, split, least, high):
    def one(dim, blocks):
        heights = jax.random.uniform(jax.random.fold_in(jax.random.fold_in(rng, 6), dim), (blocks,), jnp.float32, least / len(split), high / len(split))
        return jnp.repeat(jnp.exp(heights), dims[dim] // blocks).reshape((-1,) + (1,) * (len(dims) - dim - 1))

    factor_of = one(*split[0])
    for cut in split[1:]:
        factor_of = factor_of * one(*cut)
    return factor_of


def noise(key, shape, deviation, most, pieces=(), held_as=jnp.bfloat16):
    drawn = deviation * jax.random.normal(key, shape, jnp.float32)
    if pieces:
        drawn = drawn * levels(key, shape, pieces, -0.22, 0.18)
    return jnp.clip(drawn, -most, most).astype(held_as)


def setup_inputs(seed: int = 0) -> dict:
    key_of = jax.random.split(jax.random.key(seed), 7)
    return {
        "y_panels": noise(key_of[0], (2, PANEL, STATES), 1.0, 6.0, ((1, 16), (2, 16))),
        "tri_inverse": draw_tri_inverse(jax.random.fold_in(key_of[6], 71), 0),
        "coupling": noise(key_of[2], (PANEL, PANEL), PANEL ** -0.5, 0.1875, ((0, 16), (1, 16))),
        "rest_factor": noise(key_of[3], (REST, 2, PANEL), REST ** -0.5, 0.03125, ((0, 16),)),
        "rest_coeffs": noise(key_of[4], (REST, STATES), 1.0, 6.0, ((0, 16), (1, 16))),
        "occupations": jnp.clip(0.02 + 0.98 * jax.random.uniform(key_of[5], (STATES,), jnp.float32) ** levels(key_of[5], (STATES,), ((0, 16),), -0.2, 0.2), 0.02, 1.0),
    }


def reference(y_panels, tri_inverse, coupling, rest_factor, rest_coeffs, occupations):
    flattened = rest_factor.reshape(REST, 2 * PANEL)
    update = lax.dot_general(flattened, rest_coeffs, (((0,), (0,)), ((), ())), preferred_element_type=jnp.float32)
    update = update.reshape(2, PANEL, STATES)
    second_rhs = (y_panels[1].astype(jnp.float32) - update[1]).astype(jnp.bfloat16)
    second = jnp.dot(tri_inverse[1], second_rhs, preferred_element_type=jnp.float32).astype(jnp.bfloat16)
    cross = lax.dot_general(coupling, second, (((0,), (0,)), ((), ())), preferred_element_type=jnp.float32)
    first_rhs = (y_panels[0].astype(jnp.float32) - update[0] - cross).astype(jnp.bfloat16)
    first = jnp.dot(tri_inverse[0], first_rhs, preferred_element_type=jnp.float32).astype(jnp.bfloat16)
    panel_coeffs = jnp.stack([first, second])
    weights = occupations * (1.0 / math.sqrt(STATES))
    scaled = (first[:STRIP].astype(jnp.float32) * weights[None, :]).astype(jnp.bfloat16)
    density = lax.dot_general(rest_coeffs, scaled, (((1,), (1,)), ((), ())), preferred_element_type=jnp.float32)
    return (panel_coeffs, density.astype(jnp.bfloat16))
```

```python
import jax
import jax.numpy as jnp
from jax import lax
from jax.experimental import pallas as pl
from jax.experimental.pallas import tpu as pltpu
from jax.sharding import PartitionSpec as P

MESH = pl.DeviceIdType.MESH
BF16 = jnp.bfloat16
F32 = jnp.float32
NZ = 8
SIDE = 4
KB = 256
CHUNKS = ((1, 0), (1, 1), (0, 0), (0, 1))
WIDE = 512


def iota(shape, dim):
    return lax.broadcasted_iota(jnp.int32, shape, dim)


def kernel(
    y_ref, tri_ref, coup_ref, fac_ref, rc_ref, occ_ref,
    panel_ref, dens_ref,
    fbuf, rci, tsend, trecv, tg, ownf, psend, precv, zsend, zrecv,
    sc, rca, rcb, pa, pb, paf, pbf, ra, rb, po, pr, turn,
    fsem, send_sem, recv_sem,
):
    r = lax.axis_index("row")
    c = lax.axis_index("col")
    z, core = r // 2, r % 2
    y, x = c // SIDE, c % SIDE
    rest = rc_ref.shape[0]
    count = [0]
    started = []

    def zdev(d, other=0):
        k = core if not other else 1 - core
        return (lax.rem(z + d, NZ) * 2 + k, c)

    def xcol(d):
        return y * SIDE + lax.rem(x + d, SIDE)

    def ycol(d):
        return lax.rem(y + d, SIDE) * SIDE + x

    def copy(src, dst, dev):
        k = count[0]
        count[0] += 1
        made = pltpu.make_async_remote_copy(
            src_ref=src, dst_ref=dst, send_sem=send_sem.at[k], recv_sem=recv_sem.at[k],
            device_id=dev, device_id_type=MESH,
        )
        made.start()
        started.append(made)
        return made

    partner = zdev(0, 1)

    loads = []
    for nb in range(8):
        load = pltpu.make_async_copy(
            fac_ref.at[:, :, pl.ds(nb * 128, 128)], fbuf.at[nb], fsem.at[nb]
        )
        loads.append(load)
    for nb in range(8):
        loads[nb].start()

    barrier = pltpu.get_barrier_semaphore()
    greeted = [partner]
    for d in range(1, NZ):
        greeted += [zdev(d), zdev(d, 1)]
    for d in range(1, SIDE):
        greeted += [(r, xcol(d)), (r, ycol(d))]
    for dev in greeted:
        pl.semaphore_signal(barrier, inc=1, device_id=dev, device_id_type=MESH)

    for m in range(3):
        block = (coup_ref[...] if m == 2 else tri_ref[m]).astype(F32).T.astype(BF16)
        tsend[m] = jnp.concatenate([block, block], axis=1)

    krow, kcol = iota((KB, 2 * KB), 0), iota((KB, 2 * KB), 1)
    spread = [jnp.where(kcol == 2 * krow + p, -1.0, 0.0).astype(BF16) for p in range(2)]

    def widen(kb, carry):
        turned = rc_ref[pl.ds(pl.multiple_of(kb * KB, KB), KB), :].T
        for p in range(2):
            rci[p, :, pl.ds(pl.multiple_of(kb * 2 * KB, 2 * KB), 2 * KB)] = jnp.dot(
                turned, spread[p], preferred_element_type=F32
            ).astype(BF16)
        return carry

    lax.fori_loop(0, rest // KB, widen, 0)

    pl.semaphore_wait(barrier, len(greeted))
    t_pair = copy(tsend, trecv, partner)

    def product(k):
        p, q = CHUNKS[k]
        if p == 1:
            for nb in range(4 * q, 4 * q + 4):
                loads[nb].wait()
        turned = y_ref[p].astype(F32).T.astype(BF16)
        here = core == 0

        def columns(n, carry):
            base = q * WIDE + n * 256
            place = (iota((64, 256), 1) + base == r * 64 + iota((64, 256), 0)).astype(F32)
            w = jnp.concatenate(
                [fbuf[4 * q + 2 * n + i].reshape(2 * rest, 128) for i in range(2)], axis=1
            )
            got = jnp.dot(rci[p], w, preferred_element_type=F32) + jnp.dot(
                turned, place.astype(BF16), preferred_element_type=F32
            )
            low, high = got[:128], got[128:]
            lanes = pl.ds(pl.multiple_of(n * 256, 256), 256)
            ownf[k, :, lanes] = jnp.where(here, low, high)
            psend[k, :, lanes] = jnp.where(here, high, low).astype(BF16)
            return carry

        lax.fori_loop(0, 2, columns, 0)
        return copy(psend.at[k], precv.at[k], partner)

    def combine(k, pair):
        pair.wait_recv()
        total = ownf[k] + precv[k].astype(F32)
        ownf[k] = total
        zsend[k] = total.astype(BF16).reshape(NZ, 16, WIDE)
        out = []
        for d in (4, 3, 5, 2, 6, 1, 7):
            out.append(copy(zsend.at[k, lax.rem(z + d, NZ)], zrecv.at[k, d], zdev(d)))
        return out

    pairs, zs = [], []
    pairs.append(product(0))

    t_pair.wait_recv()
    mine = (iota((32, 128), 1) // 64) == core
    for m in range(3):
        rows = pl.ds(core * 32, 32)
        tg[core, c, z, m] = jnp.where(
            mine, tsend[m, rows, :].astype(F32), trecv[m, rows, :].astype(F32)
        ).astype(BF16)
    t_z = [copy(tg.at[core, c, z], tg.at[core, c, z], zdev(d)) for d in (4, 3, 5, 2, 6, 1, 7)]

    pairs.append(product(1))
    zs.append(combine(0, pairs[0]))
    pairs.append(product(2))
    zs.append(combine(1, pairs[1]))

    for made in t_z:
        made.wait_recv()
    is0 = core == 0

    def slab(a, b):
        dx, dy = jnp.where(is0, a, b), jnp.where(is0, b, a)
        return lax.rem(y + dy, SIDE) * SIDE + lax.rem(x + dx, SIDE)

    t_a = [copy(tg.at[core, c], tg.at[core, c], (r, slab(d, 0))) for d in (2, 1, 3)]
    t_b = []
    for d in (2, 1, 3):
        t_b.append((d, 0, copy(tg.at[core, c], tg.at[core, c], (r, slab(0, d)))))

    pairs.append(product(3))
    zs.append(combine(2, pairs[2]))
    zs.append(combine(3, pairs[3]))

    t_d = [copy(tg.at[core, c], tg.at[core, c], partner)]
    for e, made in zip((2, 1, 3), t_a):
        made.wait_recv()
        came = slab(SIDE - e, 0)
        for d in (2, 1, 3):
            t_b.append((d, e, copy(tg.at[core, came], tg.at[core, came], (r, slab(0, d)))))
        t_d.append(copy(tg.at[core, came], tg.at[core, came], partner))

    view = rc_ref.reshape(SIDE, SIDE, 2, 80, 256)
    rc_x, rc_y = [], []
    for d in (2, 1, 3):
        rc_x.append(copy(view.at[:, lax.rem(x + d, SIDE), 0], rca.at[d], (r, xcol(d))))
        rc_y.append(copy(view.at[lax.rem(y + d, SIDE), :, 1], rcb.at[d], (r, ycol(d))))

    for d, e, made in t_b:
        made.wait_recv()
        came = slab((SIDE - e) % SIDE, SIDE - d)
        t_d.append(copy(tg.at[core, came], tg.at[core, came], partner))

    def rhs(p):
        parts = []
        for q in range(2):
            k = CHUNKS.index((p, q))
            for made in zs[k]:
                made.wait_recv()
            total = ownf[k, pl.ds(z * 16, 16), :]
            for d in range(1, NZ):
                total = total + zrecv[k, d].astype(F32)
            parts.append(total)
        return jnp.concatenate(parts, axis=1)

    def tile(m, kb, zs_):
        cols = []
        for zz in zs_:
            cols.append(
                jnp.concatenate(
                    [tg[h, cc, zz, m] for cc in range(4 * kb, 4 * kb + 4) for h in range(2)], axis=0
                )
            )
        return jnp.concatenate(cols, axis=1)

    def upper(m, value, q):
        total = None
        for kb in range(q, 4):
            part = jnp.dot(
                value[:, kb * 256:(kb + 1) * 256], tile(m, kb, (2 * q, 2 * q + 1)),
                preferred_element_type=F32,
            )
            total = part if total is None else total + part
        return total

    rhs1 = rhs(1).astype(BF16)
    for made in t_d:
        made.wait_recv()
    second = jnp.concatenate([upper(1, rhs1, q) for q in range(4)], axis=1).astype(BF16)
    cross = jnp.concatenate(
        [
            lax.dot_general(
                second, tile(2, kb, range(8)), (((1,), (1,)), ((), ())), preferred_element_type=F32
            )
            for kb in range(4)
        ],
        axis=1,
    )
    rhs0 = (rhs(0) - cross).astype(BF16)
    strip = jnp.concatenate([upper(0, rhs0, q) for q in range(2)], axis=1).astype(BF16)

    lane = iota((16, 256), 1)
    wanted = core * 128 + z * 16 + iota((16, 256), 0)
    weight = jnp.sum(jnp.where(lane == wanted, occ_ref[...], 0.0), axis=1, keepdims=True)
    sc[0, core, z] = (strip.astype(F32) * (weight * 0.015625)).astype(BF16)

    s_z, s_x, s_y = [], [], []
    for d in (1, 7, 2, 6, 3, 5, 4):
        s_z.append((d, copy(sc.at[0, core, z], sc.at[0, core, z], zdev(d))))

    def spread_out(zz):
        for d in (2, 1, 3):
            s_x.append(copy(sc.at[0, core, zz], sc.at[d, core, zz], (r, xcol(d))))
            s_y.append(copy(sc.at[0, core, zz], sc.at[3 + d, core, zz], (r, ycol(d))))

    spread_out(z)

    tail = jnp.concatenate([upper(0, rhs0, q) for q in range(2, 4)], axis=1).astype(BF16)
    first = jnp.concatenate([strip, tail], axis=1)
    for zz in range(NZ):
        po[zz, 0] = first[:, zz * 128:(zz + 1) * 128]
        po[zz, 1] = second[:, zz * 128:(zz + 1) * 128]
    pr[core, z] = po[z]

    for d, made in s_z:
        made.wait_recv()
        spread_out(lax.rem(z + NZ - d, NZ))
    s_d = [copy(sc.at[0, core], sc.at[0, core], partner)]

    p_out = []
    for d in range(NZ):
        for other in range(2):
            if d or other:
                dev = zdev(d, other)
                p_out.append(copy(po.at[lax.rem(z + d, NZ)], pr.at[core, z], dev))

    for g, made in zip((2, 1, 3) * NZ, s_x):
        made.wait_recv()
    for g in (2, 1, 3):
        s_d.append(copy(sc.at[g, core], sc.at[g, core], partner))
    for g, made in zip((2, 1, 3) * NZ, s_y):
        made.wait_recv()
    for g in (2, 1, 3):
        s_d.append(copy(sc.at[3 + g, core], sc.at[3 + g, core], partner))
    for made in rc_x:
        made.wait_recv()
    for made in s_d:
        made.wait_recv()
    total = jnp.dot(view[:, x, 0].reshape(320, 256), sc[0].reshape(256, 512), preferred_element_type=F32)
    for d in range(1, SIDE):
        total = total + jnp.dot(
            rca[d].reshape(320, 256), sc[d].reshape(256, 512), preferred_element_type=F32
        )
    paf[...] = total.reshape(SIDE, 80, 512)
    pa[...] = total.astype(BF16).reshape(SIDE, 80, 512)
    r_y = [copy(pa.at[lax.rem(y + d, SIDE)], ra.at[d], (r, ycol(d))) for d in (2, 1, 3)]
    for made in rc_y:
        made.wait_recv()
    total = jnp.dot(view[y, :, 1].reshape(320, 256), sc[0].reshape(256, 512), preferred_element_type=F32)
    for d in range(1, SIDE):
        total = total + jnp.dot(
            rcb[d].reshape(320, 256), sc[3 + d].reshape(256, 512), preferred_element_type=F32
        )
    pbf[...] = total.reshape(SIDE, 80, 512)
    pb[...] = total.astype(BF16).reshape(SIDE, 80, 512)
    r_x = [copy(pb.at[lax.rem(x + d, SIDE)], rb.at[d], (r, xcol(d))) for d in (2, 1, 3)]

    for made in p_out:
        made.wait_recv()
    for p in range(2):
        states = jnp.concatenate([pr[k, zz, p] for k in range(2) for zz in range(NZ)], axis=0)
        turn[p] = states.astype(F32).T
        panel_ref[p] = turn[p, pl.ds(core * 64, 64), :].astype(BF16)

    for made in r_y:
        made.wait_recv()
    total = paf[y]
    for d in range(1, SIDE):
        total = total + ra[d].astype(F32)
    dens_ref[pl.ds(0, 80), :] = total.astype(BF16)
    for made in r_x:
        made.wait_recv()
    total = pbf[x]
    for d in range(1, SIDE):
        total = total + rb[d].astype(F32)
    dens_ref[pl.ds(80, 80), :] = total.astype(BF16)

    for made in started:
        made.wait_send()


def body(y_panels, tri_inverse, coupling, rest_factor, rest_coeffs, occupations):
    rest = rest_coeffs.shape[0]
    vmem = pl.BlockSpec(memory_space=pltpu.VMEM)
    anywhere = pl.BlockSpec(memory_space=pl.ANY)
    copies = 180
    return pl.pallas_call(
        kernel,
        out_shape=(
            jax.ShapeDtypeStruct((2, 64, 256), BF16),
            jax.ShapeDtypeStruct((160, 512), BF16),
        ),
        in_specs=[vmem, vmem, vmem, anywhere, vmem, vmem],
        out_specs=(vmem, vmem),
        scratch_shapes=[
            pltpu.VMEM((8, rest, 2, 128), BF16),
            pltpu.VMEM((2, 256, 2 * rest), BF16),
            pltpu.VMEM((3, 64, 128), BF16),
            pltpu.VMEM((3, 64, 128), BF16),
            pltpu.VMEM((2, 16, NZ, 3, 32, 128), BF16),
            pltpu.VMEM((4, 128, WIDE), F32),
            pltpu.VMEM((4, 128, WIDE), BF16),
            pltpu.VMEM((4, 128, WIDE), BF16),
            pltpu.VMEM((4, NZ, 16, WIDE), BF16),
            pltpu.VMEM((4, NZ, 16, WIDE), BF16),
            pltpu.VMEM((7, 2, NZ, 16, 512), BF16),
            pltpu.VMEM((SIDE, SIDE, 80, 256), BF16),
            pltpu.VMEM((SIDE, SIDE, 80, 256), BF16),
            pltpu.VMEM((SIDE, 80, 512), BF16),
            pltpu.VMEM((SIDE, 80, 512), BF16),
            pltpu.VMEM((SIDE, 80, 512), F32),
            pltpu.VMEM((SIDE, 80, 512), F32),
            pltpu.VMEM((SIDE, 80, 512), BF16),
            pltpu.VMEM((SIDE, 80, 512), BF16),
            pltpu.VMEM((NZ, 2, 16, 128), BF16),
            pltpu.VMEM((2, NZ, 2, 16, 128), BF16),
            pltpu.VMEM((2, 128, 256), F32),
            pltpu.SemaphoreType.DMA((8,)),
            pltpu.SemaphoreType.DMA((copies,)),
            pltpu.SemaphoreType.DMA((copies,)),
        ],
        compiler_params=pltpu.CompilerParams(
            collective_id=0, has_side_effects=True, vmem_limit_bytes=60 * 1024 * 1024
        ),
    )(y_panels, tri_inverse, coupling, rest_factor, rest_coeffs, occupations.reshape(1, 256))


def solution(mesh):
    return jax.shard_map(
        body,
        mesh=mesh,
        in_specs=(
            P(None, "row", "col"),
            P(None, "row", "col"),
            P("row", "col"),
            P("row", None, None),
            P("row", "col"),
            P("col"),
        ),
        out_specs=(P(None, "row", "col"), P(("row", "col"), None)),
        check_vma=False,
    )
```

```python
import jax
import jax.numpy as jnp
from jax import lax
from jax.experimental import pallas as pl
from jax.experimental.pallas import tpu as pltpu
from jax.sharding import PartitionSpec as P

MESH = pl.DeviceIdType.MESH
BF16 = jnp.bfloat16
F32 = jnp.float32
NZ = 8
SIDE = 4
KB = 256
CHUNKS = ((1, 0), (1, 1), (0, 0), (0, 1))
WIDE = 512


def iota(shape, dim):
    return lax.broadcasted_iota(jnp.int32, shape, dim)


def kernel(
    y_in, tri_in, coup_in, fac_ref, rc_in, occ_in,
    panel_ref, dens_ref,
    y_ref, tri_ref, coup_ref, rc_ref, occ_ref,
    fbuf, rci, tsend, trecv, tt, cg, ownf, psend, precv, zsend, zrecv,
    sc, rca, rcb, pa, pb, paf, pbf, ra, rb, po, pr, turn,
    fsem, send_sem, recv_sem,
):
    r = lax.axis_index("row")
    c = lax.axis_index("col")
    z, core = r // 2, r % 2
    y, x = c // SIDE, c % SIDE
    rest = rc_ref.shape[0]
    count = [0]
    started = []

    def zdev(d, other=0):
        k = core if not other else 1 - core
        return (lax.rem(z + d, NZ) * 2 + k, c)

    def xcol(d):
        return y * SIDE + lax.rem(x + d, SIDE)

    def ycol(d):
        return lax.rem(y + d, SIDE) * SIDE + x

    def copy(src, dst, dev):
        k = count[0]
        count[0] += 1
        made = pltpu.make_async_remote_copy(
            src_ref=src, dst_ref=dst, send_sem=send_sem.at[k], recv_sem=recv_sem.at[k],
            device_id=dev, device_id_type=MESH,
        )
        made.start()
        started.append(made)
        return made

    partner = zdev(0, 1)

    barrier = pltpu.get_barrier_semaphore()
    greeted = [partner]
    for d in range(1, NZ):
        greeted += [zdev(d), zdev(d, 1)]
    for d in range(1, SIDE):
        greeted += [(r, xcol(d)), (r, ycol(d))]
    for dev in greeted:
        pl.semaphore_signal(barrier, inc=1, device_id=dev, device_id_type=MESH)

    own = []
    for k, (src, dst) in enumerate(
        ((tri_in, tri_ref), (coup_in, coup_ref), (rc_in, rc_ref), (y_in, y_ref), (occ_in, occ_ref))
    ):
        own.append(pltpu.make_async_copy(src, dst, fsem.at[8 + k]))
        own[k].start()

    loads = []
    for nb in range(8):
        load = pltpu.make_async_copy(
            fac_ref.reshape(2 * rest, 1024).at[:, pl.ds(nb * 128, 128)], fbuf.at[nb], fsem.at[nb]
        )
        loads.append(load)
    for nb in range(8):
        loads[nb].start()

    own[0].wait()
    own[1].wait()
    for m in range(3):
        block = (coup_ref[...] if m == 2 else tri_ref[m]).astype(F32).T.astype(BF16)
        tsend[m] = jnp.concatenate([block, block], axis=1)

    own[2].wait()
    krow, kcol = iota((KB, 2 * KB), 0), iota((KB, 2 * KB), 1)
    spread = [jnp.where(kcol == 2 * krow + p, -1.0, 0.0).astype(BF16) for p in range(2)]

    def widen(kb, carry):
        turned = rc_ref[pl.ds(pl.multiple_of(kb * KB, KB), KB), :].T
        for p in range(2):
            rci[p, :, pl.ds(pl.multiple_of(kb * 2 * KB, 2 * KB), 2 * KB)] = jnp.dot(
                turned, spread[p], preferred_element_type=F32
            ).astype(BF16)
        return carry

    half = rest // KB // 2
    lax.fori_loop(0, half, widen, 0)

    pl.semaphore_wait(barrier, len(greeted))
    t_pair = copy(tsend, trecv, partner)

    view = rc_ref.reshape(SIDE, SIDE, 2, 80, 256)
    rc_x, rc_y = [], []

    def exchange(d):
        rc_x.append(copy(view.at[:, lax.rem(x + d, SIDE), 0], rca.at[d], (r, xcol(d))))
        rc_y.append(copy(view.at[lax.rem(y + d, SIDE), :, 1], rcb.at[d], (r, ycol(d))))

    for d in (2, 1, 3):
        exchange(d)

    def product(k):
        p, q = CHUNKS[k]
        if p == 1:
            for nb in range(4 * q, 4 * q + 4):
                loads[nb].wait()
        if k == 0:
            own[3].wait()
        turned = y_ref[p].astype(F32).T.astype(BF16)
        here = core == 0

        def columns(n, carry):
            base = q * WIDE + n * 256
            place = (iota((64, 256), 1) + base == r * 64 + iota((64, 256), 0)).astype(F32)
            w = jnp.concatenate([fbuf[4 * q + 2 * n + i] for i in range(2)], axis=1)
            got = jnp.dot(rci[p], w, preferred_element_type=F32) + jnp.dot(
                turned, place.astype(BF16), preferred_element_type=F32
            )
            low, high = got[:128], got[128:]
            lanes = pl.ds(pl.multiple_of(n * 256, 256), 256)
            ownf[k, :, lanes] = jnp.where(here, low, high)
            psend[k, :, lanes] = jnp.where(here, high, low).astype(BF16)
            return carry

        lax.fori_loop(0, 2, columns, 0)
        return copy(psend.at[k], precv.at[k], partner)

    def combine(k, pair):
        pair.wait_recv()
        total = ownf[k] + precv[k].astype(F32)
        ownf[k] = total
        zsend[k] = total.astype(BF16).reshape(NZ, 16, WIDE)
        out = []
        for d in (4, 3, 5, 2, 6, 1, 7):
            out.append(copy(zsend.at[k, lax.rem(z + d, NZ)], zrecv.at[k, d], zdev(d)))
        return out

    pairs, zs = [], []
    is0 = core == 0

    class Upper:
        def __init__(self, cc, to, out, come):
            k = count[0]
            count[0] += 1
            self.out, self.come = out, come
            self.made = [
                pltpu.make_async_remote_copy(
                    src_ref=tt.at[core, cc, pl.ds(0, 2 * v + 2)],
                    dst_ref=tt.at[core, cc, pl.ds(0, 2 * v + 2)],
                    send_sem=send_sem.at[k], recv_sem=recv_sem.at[k],
                    device_id=to, device_id_type=MESH,
                )
                for v in range(SIDE)
            ]
            for v in range(SIDE):
                pl.when(out == v)(self.made[v].start)
            started.append(self)

        def wait_recv(self):
            for v in range(SIDE):
                pl.when(self.come == v)(self.made[v].wait_recv)

        def wait_send(self):
            for v in range(SIDE):
                pl.when(self.out == v)(self.made[v].wait_send)

    def whole(cc, to):
        return copy(cg.at[core, cc], cg.at[core, cc], to)

    class Maybe:
        def __init__(self, src, dst, to, out, come):
            k = count[0]
            count[0] += 1
            self.out, self.come = out, come
            self.made = pltpu.make_async_remote_copy(
                src_ref=src, dst_ref=dst, send_sem=send_sem.at[k], recv_sem=recv_sem.at[k],
                device_id=to, device_id_type=MESH,
            )
            pl.when(out)(self.made.start)
            started.append(self)

        def wait_recv(self):
            pl.when(self.come)(self.made.wait_recv)

        def wait_send(self):
            pl.when(self.out)(self.made.wait_send)

    t_pair.wait_recv()
    mine = (iota((32, 128), 1) // 64) == core
    for m in range(3):
        rows = pl.ds(core * 32, 32)
        got = jnp.where(
            mine, tsend[m, rows, :].astype(F32), trecv[m, rows, :].astype(F32)
        ).astype(BF16)
        if m == 2:
            cg[core, c, z] = got
        else:
            tt[core, c, z, m] = got
    t_z = []
    for d in (4, 3, 5, 2, 6, 1, 7):
        t_z.append(copy(cg.at[core, c, z], cg.at[core, c, z], zdev(d)))
        t_z.append(
            Maybe(
                tt.at[core, c, z], tt.at[core, c, z], zdev(d),
                z <= 2 * y + 1, lax.rem(z + NZ - d, NZ) <= 2 * y + 1,
            )
        )

    def moved(a, b):
        dx, dy = jnp.where(is0, a, b), jnp.where(is0, b, a)
        return lax.rem(x + dx, SIDE), lax.rem(y + dy, SIDE)

    def slab(a, b):
        xx, yy = moved(a, b)
        return yy * SIDE + xx

    def behind(e, d):
        back = ((SIDE - e) % SIDE, (SIDE - d) % SIDE)
        return slab(*back), moved(*back)[1], moved(*back[::-1])[1]

    def to_axis_b(e):
        cc, out, _ = behind(e, 0)
        for d in (1, 3):
            to = (r, slab(0, d))
            t_b[e, d] = (Upper(cc, to, out, behind(e, d)[1]), whole(cc, to))
        to_partner(e, 0)

    def onward(e):
        for made in t_b[e, 1] + t_b[e, 3]:
            made.wait_recv()
        far = behind(e, 2)[1]
        t_far[e] = (
            Upper(behind(e, 3)[0], (r, slab(0, 3)), behind(e, 3)[1], far),
            whole(behind(e, 1)[0], (r, slab(0, 1))),
        )
        to_partner(e, 1)
        to_partner(e, 3)

    def to_partner(e, d):
        cc, out, come = behind(e, d)
        t_d.append(Upper(cc, partner, out, come))
        t_d.append(whole(cc, partner))

    lax.fori_loop(half, rest // KB, widen, 0)
    pairs.append(product(0))
    pairs.append(product(1))

    for made in t_z:
        made.wait_recv()
    t_a, t_b, t_far, t_d = {}, {}, {}, []
    for d in (1, 3, 2):
        to = (r, slab(d, 0))
        t_a[d] = (Upper(c, to, y, behind(d, 0)[1]), whole(c, to))

    zs.append(combine(0, pairs[0]))
    zs.append(combine(1, pairs[1]))
    pairs.append(product(2))
    pairs.append(product(3))
    to_axis_b(0)
    zs.append(combine(2, pairs[2]))

    for e in (1, 3, 2):
        for made in t_a[e]:
            made.wait_recv()
        to_axis_b(e)
        if e == 1:
            zs.append(combine(3, pairs[3]))
        if e == 3:
            onward(0)
    for e in (1, 3, 2):
        onward(e)
    for e in (0, 1, 3, 2):
        for made in t_far[e]:
            made.wait_recv()
        to_partner(e, 2)

    def rhs(p):
        parts = []
        for q in range(2):
            k = CHUNKS.index((p, q))
            for made in zs[k]:
                made.wait_recv()
            total = ownf[k, pl.ds(z * 16, 16), :]
            for d in range(1, NZ):
                total = total + zrecv[k, d].astype(F32)
            parts.append(total)
        return jnp.concatenate(parts, axis=1)

    def tile(m, kb, zs_):
        cols = []
        for zz in zs_:
            cols.append(
                jnp.concatenate(
                    [cg[h, cc, zz] if m == 2 else tt[h, cc, zz, m] for cc in range(4 * kb, 4 * kb + 4) for h in range(2)], axis=0
                )
            )
        return jnp.concatenate(cols, axis=1)

    def upper(m, value, q):
        total = None
        for kb in range(q, 4):
            part = jnp.dot(
                value[:, kb * 256:(kb + 1) * 256], tile(m, kb, (2 * q, 2 * q + 1)),
                preferred_element_type=F32,
            )
            total = part if total is None else total + part
        return total

    rhs1 = rhs(1).astype(BF16)
    for made in t_d:
        made.wait_recv()
    second = jnp.concatenate([upper(1, rhs1, q) for q in range(4)], axis=1).astype(BF16)
    cross = jnp.concatenate(
        [
            lax.dot_general(
                second, tile(2, kb, range(8)), (((1,), (1,)), ((), ())), preferred_element_type=F32
            )
            for kb in range(4)
        ],
        axis=1,
    )
    rhs0 = (rhs(0) - cross).astype(BF16)
    strip = jnp.concatenate([upper(0, rhs0, q) for q in range(2)], axis=1).astype(BF16)

    own[4].wait()
    lane = iota((16, 256), 1)
    wanted = core * 128 + z * 16 + iota((16, 256), 0)
    weight = jnp.sum(jnp.where(lane == wanted, occ_ref[...], 0.0), axis=1, keepdims=True)
    sc[0, core, z] = (strip.astype(F32) * (weight * 0.015625)).astype(BF16)

    s_z, s_x, s_y = [], [], []
    for d in (4, 3, 5, 2, 6, 1, 7):
        s_z.append((d, copy(sc.at[0, core, z], sc.at[0, core, z], zdev(d))))

    def spread_out(zz, zin):
        for d in (2, 1, 3):
            s_x.append((d, zin, copy(sc.at[0, core, zz], sc.at[d, core, zz], (r, xcol(d)))))
            s_y.append((3 + d, zin, copy(sc.at[0, core, zz], sc.at[3 + d, core, zz], (r, ycol(d)))))

    spread_out(z, z)

    tail = jnp.concatenate([upper(0, rhs0, q) for q in range(2, 4)], axis=1).astype(BF16)
    first = jnp.concatenate([strip, tail], axis=1)
    for zz in range(NZ):
        po[zz, 0] = first[:, zz * 128:(zz + 1) * 128]
        po[zz, 1] = second[:, zz * 128:(zz + 1) * 128]
    pr[core, z] = po[z]

    for d, made in s_z[::-1]:
        made.wait_recv()
        zz = lax.rem(z + NZ - d, NZ)
        spread_out(zz, zz)
    s_d = [copy(sc.at[0, core], sc.at[0, core], partner)]

    p_out = []
    for d in range(NZ):
        for other in range(2):
            if d or other:
                dev = zdev(d, other)
                p_out.append(copy(po.at[lax.rem(z + d, NZ)], pr.at[core, z], dev))

    for pair in zip(s_x, s_y):
        for g, zz, made in pair:
            made.wait_recv()
            s_d.append(copy(sc.at[g, core, zz], sc.at[g, core, zz], partner))
    for made in rc_x + rc_y + s_d:
        made.wait_recv()

    def along_y(steps):
        rows = [lax.rem(y + d, SIDE) for d in steps]
        total = 0.0
        for g in range(SIDE):
            block = jnp.concatenate([rca[g, k] if g else view[k, x, 0] for k in rows], axis=0)
            total = total + jnp.dot(block, sc[g].reshape(256, 512), preferred_element_type=F32)
        return total

    def along_x(steps):
        rows = [lax.rem(x + d, SIDE) for d in steps]
        total = 0.0
        for g in range(SIDE):
            block = jnp.concatenate([rcb[g, k] if g else view[y, k, 1] for k in rows], axis=0)
            slot = 3 + g if g else 0
            total = total + jnp.dot(block, sc[slot].reshape(256, 512), preferred_element_type=F32)
        return total

    far = (2, 1, 3)
    pa[...] = along_y(far).astype(BF16).reshape(3, 80, 512)
    r_y = [copy(pa.at[k], ra.at[d], (r, ycol(d))) for k, d in enumerate(far)]
    pb[...] = along_x(far).astype(BF16).reshape(3, 80, 512)
    r_x = [copy(pb.at[k], rb.at[d], (r, xcol(d))) for k, d in enumerate(far)]
    paf[...] = along_y((0,))
    pbf[...] = along_x((0,))

    for made in p_out:
        made.wait_recv()
    for p in range(2):
        states = jnp.concatenate([pr[k, zz, p] for k in range(2) for zz in range(NZ)], axis=0)
        turn[p] = states.astype(F32).T
        panel_ref[p] = turn[p, pl.ds(core * 64, 64), :].astype(BF16)

    for made in r_y:
        made.wait_recv()
    total = paf[...]
    for d in range(1, SIDE):
        total = total + ra[d].astype(F32)
    dens_ref[pl.ds(0, 80), :] = total.astype(BF16)
    for made in r_x:
        made.wait_recv()
    total = pbf[...]
    for d in range(1, SIDE):
        total = total + rb[d].astype(F32)
    dens_ref[pl.ds(80, 80), :] = total.astype(BF16)

    for made in started:
        made.wait_send()


def body(y_panels, tri_inverse, coupling, rest_factor, rest_coeffs, occupations):
    rest = rest_coeffs.shape[0]
    vmem = pl.BlockSpec(memory_space=pltpu.VMEM)
    anywhere = pl.BlockSpec(memory_space=pltpu.HBM)
    copies = 300
    return pl.pallas_call(
        kernel,
        out_shape=(
            jax.ShapeDtypeStruct((2, 64, 256), BF16),
            jax.ShapeDtypeStruct((160, 512), BF16),
        ),
        in_specs=[anywhere] * 6,
        out_specs=(vmem, vmem),
        scratch_shapes=[
            pltpu.VMEM((2, 64, 256), BF16),
            pltpu.VMEM((2, 64, 64), BF16),
            pltpu.VMEM((64, 64), BF16),
            pltpu.VMEM((rest, 256), BF16),
            pltpu.VMEM((1, 256), F32),
            pltpu.VMEM((8, 2 * rest, 128), BF16),
            pltpu.VMEM((2, 256, 2 * rest), BF16),
            pltpu.VMEM((3, 64, 128), BF16),
            pltpu.VMEM((3, 64, 128), BF16),
            pltpu.VMEM((2, 16, NZ, 2, 32, 128), BF16),
            pltpu.VMEM((2, 16, NZ, 32, 128), BF16),
            pltpu.VMEM((4, 128, WIDE), F32),
            pltpu.VMEM((4, 128, WIDE), BF16),
            pltpu.VMEM((4, 128, WIDE), BF16),
            pltpu.VMEM((4, NZ, 16, WIDE), BF16),
            pltpu.VMEM((4, NZ, 16, WIDE), BF16),
            pltpu.VMEM((7, 2, NZ, 16, 512), BF16),
            pltpu.VMEM((SIDE, SIDE, 80, 256), BF16),
            pltpu.VMEM((SIDE, SIDE, 80, 256), BF16),
            pltpu.VMEM((3, 80, 512), BF16),
            pltpu.VMEM((3, 80, 512), BF16),
            pltpu.VMEM((80, 512), F32),
            pltpu.VMEM((80, 512), F32),
            pltpu.VMEM((SIDE, 80, 512), BF16),
            pltpu.VMEM((SIDE, 80, 512), BF16),
            pltpu.VMEM((NZ, 2, 16, 128), BF16),
            pltpu.VMEM((2, NZ, 2, 16, 128), BF16),
            pltpu.VMEM((2, 128, 256), F32),
            pltpu.SemaphoreType.DMA((13,)),
            pltpu.SemaphoreType.DMA((copies,)),
            pltpu.SemaphoreType.DMA((copies,)),
        ],
        compiler_params=pltpu.CompilerParams(
            collective_id=0, has_side_effects=True, vmem_limit_bytes=60 * 1024 * 1024
        ),
    )(y_panels, tri_inverse, coupling, rest_factor, rest_coeffs, occupations.reshape(1, 256))


def solution(mesh):
    return jax.shard_map(
        body,
        mesh=mesh,
        in_specs=(
            P(None, "row", "col"),
            P(None, "row", "col"),
            P("row", "col"),
            P("row", None, None),
            P("row", "col"),
            P("col"),
        ),
        out_specs=(P(None, "row", "col"), P(("row", "col"), None)),
        check_vma=False,
    )
```

```python
import jax
import jax.numpy as jnp
from jax import lax
from jax.experimental import pallas as pl
from jax.experimental.pallas import tpu as pltpu
from jax.sharding import PartitionSpec as P

MESH = pl.DeviceIdType.MESH
BF16 = jnp.bfloat16
F32 = jnp.float32
NZ = 8
SIDE = 4
KB = 256
CHUNKS = ((1, 0), (1, 1), (0, 0), (0, 1))
WIDE = 512


def iota(shape, dim):
    return lax.broadcasted_iota(jnp.int32, shape, dim)


def kernel(
    y_in, tri_in, coup_in, fac_ref, rc_in, occ_in,
    panel_ref, dens_ref,
    y_ref, tri_ref, coup_ref, rc_ref, occ_ref,
    fbuf, rci, tsend, trecv, tt, cg, ownf, psend, precv, zsend, zrecv,
    sc, rca, rcb, pa, pb, paf, pbf, ra, rb, po, pr, turn,
    fsem, send_sem, recv_sem,
):
    r = lax.axis_index("row")
    c = lax.axis_index("col")
    z, core = r // 2, r % 2
    y, x = c // SIDE, c % SIDE
    rest = rc_ref.shape[0]
    count = [0]
    started = []

    def zdev(d, other=0):
        k = core if not other else 1 - core
        return (lax.rem(z + d, NZ) * 2 + k, c)

    def xcol(d):
        return y * SIDE + lax.rem(x + d, SIDE)

    def ycol(d):
        return lax.rem(y + d, SIDE) * SIDE + x

    def copy(src, dst, dev):
        k = count[0]
        count[0] += 1
        made = pltpu.make_async_remote_copy(
            src_ref=src, dst_ref=dst, send_sem=send_sem.at[k], recv_sem=recv_sem.at[k],
            device_id=dev, device_id_type=MESH,
        )
        made.start()
        started.append(made)
        return made

    partner = zdev(0, 1)

    barrier = pltpu.get_barrier_semaphore()
    greeted = [partner]
    for d in range(1, NZ):
        greeted += [zdev(d), zdev(d, 1)]
    for d in range(1, SIDE):
        greeted += [(r, xcol(d)), (r, ycol(d))]
    for dev in greeted:
        pl.semaphore_signal(barrier, inc=1, device_id=dev, device_id_type=MESH)

    own = []
    for k, (src, dst) in enumerate(
        ((tri_in, tri_ref), (coup_in, coup_ref), (rc_in, rc_ref), (y_in, y_ref), (occ_in, occ_ref))
    ):
        own.append(pltpu.make_async_copy(src, dst, fsem.at[8 + k]))
        own[k].start()

    loads = []
    for nb in range(8):
        load = pltpu.make_async_copy(
            fac_ref.reshape(2 * rest, 1024).at[:, pl.ds(nb * 128, 128)], fbuf.at[nb], fsem.at[nb]
        )
        loads.append(load)
    for nb in range(8):
        loads[nb].start()

    own[0].wait()
    own[1].wait()
    for m in range(3):
        block = (coup_ref[...] if m == 2 else tri_ref[m]).astype(F32).T.astype(BF16)
        tsend[m] = jnp.concatenate([block, block], axis=1)

    own[2].wait()
    krow, kcol = iota((KB, 2 * KB), 0), iota((KB, 2 * KB), 1)
    spread = [jnp.where(kcol == 2 * krow + p, -1.0, 0.0).astype(BF16) for p in range(2)]

    def widen(kb, carry):
        turned = rc_ref[pl.ds(pl.multiple_of(kb * KB, KB), KB), :].T
        for p in range(2):
            rci[p, :, pl.ds(pl.multiple_of(kb * 2 * KB, 2 * KB), 2 * KB)] = jnp.dot(
                turned, spread[p], preferred_element_type=F32
            ).astype(BF16)
        return carry

    half = rest // KB // 2
    lax.fori_loop(0, half, widen, 0)

    pl.semaphore_wait(barrier, len(greeted))
    t_pair = copy(tsend, trecv, partner)

    view = rc_ref.reshape(SIDE, SIDE, 2, 80, 256)
    rc_x, rc_y = [], []

    def exchange(d):
        rc_x.append(copy(view.at[:, lax.rem(x + d, SIDE), 0], rca.at[d], (r, xcol(d))))
        rc_y.append(copy(view.at[lax.rem(y + d, SIDE), :, 1], rcb.at[d], (r, ycol(d))))

    exchange(1)
    exchange(3)

    def product(k):
        p, q = CHUNKS[k]
        if p == 1:
            for nb in range(4 * q, 4 * q + 4):
                loads[nb].wait()
        if k == 0:
            own[3].wait()
        turned = y_ref[p].astype(F32).T.astype(BF16)
        here = core == 0

        def columns(n, carry):
            base = q * WIDE + n * 256
            place = (iota((64, 256), 1) + base == r * 64 + iota((64, 256), 0)).astype(F32)
            w = jnp.concatenate([fbuf[4 * q + 2 * n + i] for i in range(2)], axis=1)
            got = jnp.dot(rci[p], w, preferred_element_type=F32) + jnp.dot(
                turned, place.astype(BF16), preferred_element_type=F32
            )
            low, high = got[:128], got[128:]
            lanes = pl.ds(pl.multiple_of(n * 256, 256), 256)
            ownf[k, :, lanes] = jnp.where(here, low, high)
            psend[k, :, lanes] = jnp.where(here, high, low).astype(BF16)
            return carry

        lax.fori_loop(0, 2, columns, 0)
        return copy(psend.at[k], precv.at[k], partner)

    def combine(k, pair):
        pair.wait_recv()
        total = ownf[k] + precv[k].astype(F32)
        ownf[k] = total
        zsend[k] = total.astype(BF16).reshape(NZ, 16, WIDE)
        out = []
        for d in (4, 3, 5, 2, 6, 1, 7):
            out.append(copy(zsend.at[k, lax.rem(z + d, NZ)], zrecv.at[k, d], zdev(d)))
        return out

    pairs, zs = [], []
    is0 = core == 0

    class Upper:
        def __init__(self, cc, to, out, come, sizes=range(SIDE)):
            k = count[0]
            count[0] += 1
            self.out, self.come, self.sizes = out, come, sizes
            self.made = [
                pltpu.make_async_remote_copy(
                    src_ref=tt.at[core, cc, pl.ds(0, 2 * v + 2)],
                    dst_ref=tt.at[core, cc, pl.ds(0, 2 * v + 2)],
                    send_sem=send_sem.at[k], recv_sem=recv_sem.at[k],
                    device_id=to, device_id_type=MESH,
                )
                for v in range(SIDE)
            ]
            for v in sizes:
                pl.when(out == v)(self.made[v].start)
            started.append(self)

        def wait_recv(self):
            for v in self.sizes:
                pl.when(self.come == v)(self.made[v].wait_recv)

        def wait_send(self):
            for v in self.sizes:
                pl.when(self.out == v)(self.made[v].wait_send)

    def whole(cc, to):
        return copy(cg.at[core, cc], cg.at[core, cc], to)

    class Maybe:
        def __init__(self, src, dst, to, out, come):
            k = count[0]
            count[0] += 1
            self.out, self.come = out, come
            self.made = pltpu.make_async_remote_copy(
                src_ref=src, dst_ref=dst, send_sem=send_sem.at[k], recv_sem=recv_sem.at[k],
                device_id=to, device_id_type=MESH,
            )
            pl.when(out)(self.made.start)
            started.append(self)

        def wait_recv(self):
            pl.when(self.come)(self.made.wait_recv)

        def wait_send(self):
            pl.when(self.out)(self.made.wait_send)

    t_pair.wait_recv()
    mine = (iota((32, 128), 1) // 64) == core
    for m in range(3):
        rows = pl.ds(core * 32, 32)
        got = jnp.where(
            mine, tsend[m, rows, :].astype(F32), trecv[m, rows, :].astype(F32)
        ).astype(BF16)
        if m == 2:
            cg[core, c, z] = got
        else:
            tt[core, c, z, m] = got
    t_z = []
    for d in (4, 3, 5, 2, 6, 1, 7):
        t_z.append(copy(cg.at[core, c, z], cg.at[core, c, z], zdev(d)))
        t_z.append(
            Maybe(
                tt.at[core, c, z], tt.at[core, c, z], zdev(d),
                z <= 2 * y + 1, lax.rem(z + NZ - d, NZ) <= 2 * y + 1,
            )
        )

    def moved(a, b):
        dx, dy = jnp.where(is0, a, b), jnp.where(is0, b, a)
        return lax.rem(x + dx, SIDE), lax.rem(y + dy, SIDE)

    def slab(a, b):
        xx, yy = moved(a, b)
        return yy * SIDE + xx

    def behind(e, d):
        back = ((SIDE - e) % SIDE, (SIDE - d) % SIDE)
        return slab(*back), moved(*back)[1], moved(*back[::-1])[1]

    def to_axis_b(e):
        cc, out, _ = behind(e, 0)
        for d in (1, 3):
            to = (r, slab(0, d))
            t_b[e, d] = (Upper(cc, to, out, behind(e, d)[1]), whole(cc, to))
        to_partner(e, 0)

    def onward(e):
        for made in t_b[e, 1] + t_b[e, 3]:
            made.wait_recv()
        far = behind(e, 2)[1]
        (low, low_size, _), (high, high_size, _) = behind(e, 1), behind(e, 3)
        up, down = (r, slab(0, 1)), (r, slab(0, 3))
        last = SIDE - 1
        t_far[e] = (
            Upper(high, down, high_size, far, range(last)),
            Upper(low, up, low_size, far, (last,)),
            Maybe(cg.at[core, low], cg.at[core, low], up, low_size != last, far != last),
            Maybe(cg.at[core, high], cg.at[core, high], down, high_size == last, far == last),
        )
        to_partner(e, 1)
        to_partner(e, 3)

    def to_partner(e, d):
        cc, out, come = behind(e, d)
        t_d.append(Upper(cc, partner, out, come))
        t_d.append(whole(cc, partner))

    lax.fori_loop(half, rest // KB, widen, 0)
    pairs.append(product(0))
    pairs.append(product(1))

    for made in t_z:
        made.wait_recv()
    t_a, t_b, t_far, t_d = {}, {}, {}, []
    for d in (1, 3, 2):
        to = (r, slab(d, 0))
        t_a[d] = (Upper(c, to, y, behind(d, 0)[1]), whole(c, to))

    zs.append(combine(0, pairs[0]))
    zs.append(combine(1, pairs[1]))
    pairs.append(product(2))
    pairs.append(product(3))
    to_axis_b(0)
    zs.append(combine(2, pairs[2]))

    for e in (1, 3, 2):
        for made in t_a[e]:
            made.wait_recv()
        to_axis_b(e)
        if e == 1:
            zs.append(combine(3, pairs[3]))
        if e == 3:
            onward(0)
    for e in (1, 3, 2):
        onward(e)
    for e in (0, 1, 3, 2):
        for made in t_far[e]:
            made.wait_recv()
        to_partner(e, 2)

    def rhs(p):
        parts = []
        for q in range(2):
            k = CHUNKS.index((p, q))
            for made in zs[k]:
                made.wait_recv()
            total = ownf[k, pl.ds(z * 16, 16), :]
            for d in range(1, NZ):
                total = total + zrecv[k, d].astype(F32)
            parts.append(total)
        return jnp.concatenate(parts, axis=1)

    def tile(m, kb, zs_):
        cols = []
        for zz in zs_:
            cols.append(
                jnp.concatenate(
                    [cg[h, cc, zz] if m == 2 else tt[h, cc, zz, m] for cc in range(4 * kb, 4 * kb + 4) for h in range(2)], axis=0
                )
            )
        return jnp.concatenate(cols, axis=1)

    def upper(m, value, q):
        total = None
        for kb in range(q, 4):
            part = jnp.dot(
                value[:, kb * 256:(kb + 1) * 256], tile(m, kb, (2 * q, 2 * q + 1)),
                preferred_element_type=F32,
            )
            total = part if total is None else total + part
        return total

    rhs1 = rhs(1).astype(BF16)
    for made in t_d:
        made.wait_recv()
    exchange(2)
    second = jnp.concatenate([upper(1, rhs1, q) for q in range(4)], axis=1).astype(BF16)
    cross = jnp.concatenate(
        [
            lax.dot_general(
                second, tile(2, kb, range(8)), (((1,), (1,)), ((), ())), preferred_element_type=F32
            )
            for kb in range(4)
        ],
        axis=1,
    )
    rhs0 = (rhs(0) - cross).astype(BF16)
    strip = jnp.concatenate([upper(0, rhs0, q) for q in range(2)], axis=1).astype(BF16)

    own[4].wait()
    lane = iota((16, 256), 1)
    wanted = core * 128 + z * 16 + iota((16, 256), 0)
    weight = jnp.sum(jnp.where(lane == wanted, occ_ref[...], 0.0), axis=1, keepdims=True)
    sc[0, core, z] = (strip.astype(F32) * (weight * 0.015625)).astype(BF16)

    s_z, s_x, s_y = [], [], []
    for d in (4, 3, 5, 2, 6, 1, 7):
        s_z.append((d, copy(sc.at[0, core, z], sc.at[0, core, z], zdev(d))))

    def spread_out(zz, zin):
        for d in (2, 1, 3):
            s_x.append((d, zin, copy(sc.at[0, core, zz], sc.at[d, core, zz], (r, xcol(d)))))
            s_y.append((3 + d, zin, copy(sc.at[0, core, zz], sc.at[3 + d, core, zz], (r, ycol(d)))))

    spread_out(z, z)

    tail = jnp.concatenate([upper(0, rhs0, q) for q in range(2, 4)], axis=1).astype(BF16)
    first = jnp.concatenate([strip, tail], axis=1)
    for zz in range(NZ):
        po[zz, 0] = first[:, zz * 128:(zz + 1) * 128]
        po[zz, 1] = second[:, zz * 128:(zz + 1) * 128]
    pr[core, z] = po[z]

    for d, made in s_z[::-1]:
        made.wait_recv()
        zz = lax.rem(z + NZ - d, NZ)
        spread_out(zz, zz)
    s_d = [copy(sc.at[0, core], sc.at[0, core], partner)]

    p_out = []
    for d in range(NZ):
        for other in range(2):
            if d or other:
                dev = zdev(d, other)
                p_out.append(copy(po.at[lax.rem(z + d, NZ)], pr.at[core, z], dev))

    for pair in zip(s_x, s_y):
        for g, zz, made in pair:
            made.wait_recv()
            s_d.append(copy(sc.at[g, core, zz], sc.at[g, core, zz], partner))
    for made in rc_x + rc_y + s_d:
        made.wait_recv()

    def along_y(steps):
        rows = [lax.rem(y + d, SIDE) for d in steps]
        total = 0.0
        for g in range(SIDE):
            block = jnp.concatenate([rca[g, k] if g else view[k, x, 0] for k in rows], axis=0)
            total = total + jnp.dot(block, sc[g].reshape(256, 512), preferred_element_type=F32)
        return total

    def along_x(steps):
        rows = [lax.rem(x + d, SIDE) for d in steps]
        total = 0.0
        for g in range(SIDE):
            block = jnp.concatenate([rcb[g, k] if g else view[y, k, 1] for k in rows], axis=0)
            slot = 3 + g if g else 0
            total = total + jnp.dot(block, sc[slot].reshape(256, 512), preferred_element_type=F32)
        return total

    far = (2, 1, 3)
    pa[...] = along_y(far).astype(BF16).reshape(3, 80, 512)
    r_y = [copy(pa.at[k], ra.at[d], (r, ycol(d))) for k, d in enumerate(far)]
    pb[...] = along_x(far).astype(BF16).reshape(3, 80, 512)
    r_x = [copy(pb.at[k], rb.at[d], (r, xcol(d))) for k, d in enumerate(far)]
    paf[...] = along_y((0,))
    pbf[...] = along_x((0,))

    for made in p_out:
        made.wait_recv()
    for p in range(2):
        states = jnp.concatenate([pr[k, zz, p] for k in range(2) for zz in range(NZ)], axis=0)
        turn[p] = states.astype(F32).T
        panel_ref[p] = turn[p, pl.ds(core * 64, 64), :].astype(BF16)

    for made in r_y:
        made.wait_recv()
    total = paf[...]
    for d in range(1, SIDE):
        total = total + ra[d].astype(F32)
    dens_ref[pl.ds(0, 80), :] = total.astype(BF16)
    for made in r_x:
        made.wait_recv()
    total = pbf[...]
    for d in range(1, SIDE):
        total = total + rb[d].astype(F32)
    dens_ref[pl.ds(80, 80), :] = total.astype(BF16)

    for made in started:
        made.wait_send()


def settle(panel_in, dens_in, panel_out, dens_out, sem):
    moves = [
        pltpu.make_async_copy(panel_in, panel_out, sem.at[0]),
        pltpu.make_async_copy(dens_in, dens_out, sem.at[1]),
    ]
    for move in moves:
        move.start()
    for move in moves:
        move.wait()


def body(y_panels, tri_inverse, coupling, rest_factor, rest_coeffs, occupations):
    rest = rest_coeffs.shape[0]
    vmem = pl.BlockSpec(memory_space=pltpu.VMEM)
    anywhere = pl.BlockSpec(memory_space=pltpu.HBM)
    copies = 300
    shapes = (
        jax.ShapeDtypeStruct((2, 64, 256), BF16),
        jax.ShapeDtypeStruct((160, 512), BF16),
    )
    results = pl.pallas_call(
        kernel,
        out_shape=shapes,
        in_specs=[anywhere] * 6,
        out_specs=(vmem, vmem),
        scratch_shapes=[
            pltpu.VMEM((2, 64, 256), BF16),
            pltpu.VMEM((2, 64, 64), BF16),
            pltpu.VMEM((64, 64), BF16),
            pltpu.VMEM((rest, 256), BF16),
            pltpu.VMEM((1, 256), F32),
            pltpu.VMEM((8, 2 * rest, 128), BF16),
            pltpu.VMEM((2, 256, 2 * rest), BF16),
            pltpu.VMEM((3, 64, 128), BF16),
            pltpu.VMEM((3, 64, 128), BF16),
            pltpu.VMEM((2, 16, NZ, 2, 32, 128), BF16),
            pltpu.VMEM((2, 16, NZ, 32, 128), BF16),
            pltpu.VMEM((4, 128, WIDE), F32),
            pltpu.VMEM((4, 128, WIDE), BF16),
            pltpu.VMEM((4, 128, WIDE), BF16),
            pltpu.VMEM((4, NZ, 16, WIDE), BF16),
            pltpu.VMEM((4, NZ, 16, WIDE), BF16),
            pltpu.VMEM((7, 2, NZ, 16, 512), BF16),
            pltpu.VMEM((SIDE, SIDE, 80, 256), BF16),
            pltpu.VMEM((SIDE, SIDE, 80, 256), BF16),
            pltpu.VMEM((3, 80, 512), BF16),
            pltpu.VMEM((3, 80, 512), BF16),
            pltpu.VMEM((80, 512), F32),
            pltpu.VMEM((80, 512), F32),
            pltpu.VMEM((SIDE, 80, 512), BF16),
            pltpu.VMEM((SIDE, 80, 512), BF16),
            pltpu.VMEM((NZ, 2, 16, 128), BF16),
            pltpu.VMEM((2, NZ, 2, 16, 128), BF16),
            pltpu.VMEM((2, 128, 256), F32),
            pltpu.SemaphoreType.DMA((13,)),
            pltpu.SemaphoreType.DMA((copies,)),
            pltpu.SemaphoreType.DMA((copies,)),
        ],
        compiler_params=pltpu.CompilerParams(
            collective_id=0, has_side_effects=True, vmem_limit_bytes=60 * 1024 * 1024
        ),
    )(y_panels, tri_inverse, coupling, rest_factor, rest_coeffs, occupations.reshape(1, 256))
    return pl.pallas_call(
        settle,
        out_shape=shapes,
        in_specs=[vmem, vmem],
        out_specs=(anywhere, anywhere),
        scratch_shapes=[pltpu.SemaphoreType.DMA((2,))],
        compiler_params=pltpu.CompilerParams(vmem_limit_bytes=60 * 1024 * 1024),
    )(*results)


def solution(mesh):
    return jax.shard_map(
        body,
        mesh=mesh,
        in_specs=(
            P(None, "row", "col"),
            P(None, "row", "col"),
            P("row", "col"),
            P("row", None, None),
            P("row", "col"),
            P("col"),
        ),
        out_specs=(P(None, "row", "col"), P(("row", "col"), None)),
        check_vma=False,
    )
```

```python
import jax
import jax.numpy as jnp
from jax import lax
from jax.experimental import pallas as pl
from jax.experimental.pallas import tpu as pltpu
from jax.sharding import PartitionSpec as P

MESH = pl.DeviceIdType.MESH
BF16 = jnp.bfloat16
F32 = jnp.float32
NZ = 8
SIDE = 4
KB = 256
CHUNKS = ((1, 0), (1, 1), (0, 0), (0, 1))
WIDE = 512


def iota(shape, dim):
    return lax.broadcasted_iota(jnp.int32, shape, dim)


def kernel(
    y_in, tri_in, coup_in, fac_ref, rc_in, occ_in,
    panel_ref, dens_ref,
    y_ref, tri_ref, coup_ref, rc_ref, occ_ref,
    fbuf, rci, tsend, trecv, tt, cg, ownf, psend, precv, zsend, zrecv,
    sc, rca, rcb, pa, pb, paf, pbf, ra, rb, po, pr, turn,
    fsem, send_sem, recv_sem,
):
    r = lax.axis_index("row")
    c = lax.axis_index("col")
    z, core = r // 2, r % 2
    y, x = c // SIDE, c % SIDE
    rest = rc_ref.shape[0]
    count = [0]
    started = []

    def zdev(d, other=0):
        k = core if not other else 1 - core
        return (lax.rem(z + d, NZ) * 2 + k, c)

    def xcol(d):
        return y * SIDE + lax.rem(x + d, SIDE)

    def ycol(d):
        return lax.rem(y + d, SIDE) * SIDE + x

    def copy(src, dst, dev):
        k = count[0]
        count[0] += 1
        made = pltpu.make_async_remote_copy(
            src_ref=src, dst_ref=dst, send_sem=send_sem.at[k], recv_sem=recv_sem.at[k],
            device_id=dev, device_id_type=MESH,
        )
        made.start()
        started.append(made)
        return made

    partner = zdev(0, 1)

    barrier = pltpu.get_barrier_semaphore()
    greeted = [partner]
    for d in range(1, NZ):
        greeted += [zdev(d), zdev(d, 1)]
    for d in range(1, SIDE):
        greeted += [(r, xcol(d)), (r, ycol(d))]
    for dev in greeted:
        pl.semaphore_signal(barrier, inc=1, device_id=dev, device_id_type=MESH)

    own = []
    for k, (src, dst) in enumerate(
        ((tri_in, tri_ref), (coup_in, coup_ref), (rc_in, rc_ref), (y_in, y_ref), (occ_in, occ_ref))
    ):
        own.append(pltpu.make_async_copy(src, dst, fsem.at[8 + k]))
        own[k].start()

    loads = []
    for nb in range(8):
        load = pltpu.make_async_copy(
            fac_ref.reshape(2 * rest, 1024).at[:, pl.ds(nb * 128, 128)], fbuf.at[nb], fsem.at[nb]
        )
        loads.append(load)
    for nb in range(8):
        loads[nb].start()

    own[0].wait()
    own[1].wait()
    for m in range(3):
        block = (coup_ref[...] if m == 2 else tri_ref[m]).astype(F32).T.astype(BF16)
        tsend[m] = jnp.concatenate([block, block], axis=1)

    own[2].wait()
    krow, kcol = iota((KB, 2 * KB), 0), iota((KB, 2 * KB), 1)
    spread = [jnp.where(kcol == 2 * krow + p, -1.0, 0.0).astype(BF16) for p in range(2)]

    def widen(kb, carry):
        turned = rc_ref[pl.ds(pl.multiple_of(kb * KB, KB), KB), :].T
        for p in range(2):
            rci[p, :, pl.ds(pl.multiple_of(kb * 2 * KB, 2 * KB), 2 * KB)] = jnp.dot(
                turned, spread[p], preferred_element_type=F32
            ).astype(BF16)
        return carry

    half = rest // KB // 2
    lax.fori_loop(0, half, widen, 0)

    pl.semaphore_wait(barrier, len(greeted))
    t_pair = copy(tsend, trecv, partner)

    view = rc_ref.reshape(SIDE, SIDE, 2, 80, 256)
    rc_x, rc_y = [], []

    def exchange(d):
        rc_x.append(copy(view.at[:, lax.rem(x + d, SIDE), 0], rca.at[d], (r, xcol(d))))
        rc_y.append(copy(view.at[lax.rem(y + d, SIDE), :, 1], rcb.at[d], (r, ycol(d))))

    for d in (2, 1, 3):
        exchange(d)

    def product(k):
        p, q = CHUNKS[k]
        if p == 1:
            for nb in range(4 * q, 4 * q + 4):
                loads[nb].wait()
        if k == 0:
            own[3].wait()
        turned = y_ref[p].astype(F32).T.astype(BF16)
        here = core == 0

        def columns(n, carry):
            base = q * WIDE + n * 256
            place = (iota((64, 256), 1) + base == r * 64 + iota((64, 256), 0)).astype(F32)
            w = jnp.concatenate([fbuf[4 * q + 2 * n + i] for i in range(2)], axis=1)
            got = jnp.dot(rci[p], w, preferred_element_type=F32) + jnp.dot(
                turned, place.astype(BF16), preferred_element_type=F32
            )
            low, high = got[:128], got[128:]
            lanes = pl.ds(pl.multiple_of(n * 256, 256), 256)
            ownf[k, :, lanes] = jnp.where(here, low, high)
            psend[k, :, lanes] = jnp.where(here, high, low).astype(BF16)
            return carry

        lax.fori_loop(0, 2, columns, 0)
        return copy(psend.at[k], precv.at[k], partner)

    def combine(k, pair):
        pair.wait_recv()
        total = ownf[k] + precv[k].astype(F32)
        ownf[k] = total
        zsend[k] = total.astype(BF16).reshape(NZ, 16, WIDE)
        out = []
        for d in (4, 3, 5, 2, 6, 1, 7):
            out.append(copy(zsend.at[k, lax.rem(z + d, NZ)], zrecv.at[k, d], zdev(d)))
        return out

    pairs, zs = [], []
    is0 = core == 0

    class Upper:
        def __init__(self, cc, to, out, come, sizes=range(SIDE)):
            k = count[0]
            count[0] += 1
            self.out, self.come, self.sizes = out, come, sizes
            self.made = [
                pltpu.make_async_remote_copy(
                    src_ref=tt.at[core, cc, pl.ds(0, 2 * v + 2)],
                    dst_ref=tt.at[core, cc, pl.ds(0, 2 * v + 2)],
                    send_sem=send_sem.at[k], recv_sem=recv_sem.at[k],
                    device_id=to, device_id_type=MESH,
                )
                for v in range(SIDE)
            ]
            for v in sizes:
                pl.when(out == v)(self.made[v].start)
            started.append(self)

        def wait_recv(self):
            for v in self.sizes:
                pl.when(self.come == v)(self.made[v].wait_recv)

        def wait_send(self):
            for v in self.sizes:
                pl.when(self.out == v)(self.made[v].wait_send)

    def whole(cc, to):
        return copy(cg.at[core, cc], cg.at[core, cc], to)

    class Maybe:
        def __init__(self, src, dst, to, out, come):
            k = count[0]
            count[0] += 1
            self.out, self.come = out, come
            self.made = pltpu.make_async_remote_copy(
                src_ref=src, dst_ref=dst, send_sem=send_sem.at[k], recv_sem=recv_sem.at[k],
                device_id=to, device_id_type=MESH,
            )
            pl.when(out)(self.made.start)
            started.append(self)

        def wait_recv(self):
            pl.when(self.come)(self.made.wait_recv)

        def wait_send(self):
            pl.when(self.out)(self.made.wait_send)

    t_pair.wait_recv()
    mine = (iota((32, 128), 1) // 64) == core
    for m in range(3):
        rows = pl.ds(core * 32, 32)
        got = jnp.where(
            mine, tsend[m, rows, :].astype(F32), trecv[m, rows, :].astype(F32)
        ).astype(BF16)
        if m == 2:
            cg[core, c, z] = got
        else:
            tt[core, c, z, m] = got
    t_z = []
    for d in (4, 3, 5, 2, 6, 1, 7):
        t_z.append(copy(cg.at[core, c, z], cg.at[core, c, z], zdev(d)))
        t_z.append(
            Maybe(
                tt.at[core, c, z], tt.at[core, c, z], zdev(d),
                z <= 2 * y + 1, lax.rem(z + NZ - d, NZ) <= 2 * y + 1,
            )
        )

    def moved(a, b):
        dx, dy = jnp.where(is0, a, b), jnp.where(is0, b, a)
        return lax.rem(x + dx, SIDE), lax.rem(y + dy, SIDE)

    def slab(a, b):
        xx, yy = moved(a, b)
        return yy * SIDE + xx

    def behind(e, d):
        back = ((SIDE - e) % SIDE, (SIDE - d) % SIDE)
        return slab(*back), moved(*back)[1], moved(*back[::-1])[1]

    def to_axis_b(e):
        cc, out, _ = behind(e, 0)
        for d in (1, 3):
            to = (r, slab(0, d))
            t_b[e, d] = (Upper(cc, to, out, behind(e, d)[1]), whole(cc, to))
        to_partner(e, 0)

    def onward(e):
        for made in t_b[e, 1] + t_b[e, 3]:
            made.wait_recv()
        far = behind(e, 2)[1]
        (low, low_size, _), (high, high_size, _) = behind(e, 1), behind(e, 3)
        up, down = (r, slab(0, 1)), (r, slab(0, 3))
        last = SIDE - 1
        t_far[e] = (
            Upper(high, down, high_size, far, range(last)),
            Upper(low, up, low_size, far, (last,)),
            Maybe(cg.at[core, low], cg.at[core, low], up, low_size != last, far != last),
            Maybe(cg.at[core, high], cg.at[core, high], down, high_size == last, far == last),
        )
        to_partner(e, 1)
        to_partner(e, 3)

    def to_partner(e, d):
        cc, out, come = behind(e, d)
        t_d.append(Upper(cc, partner, out, come))
        t_d.append(whole(cc, partner))

    lax.fori_loop(half, rest // KB, widen, 0)
    pairs.append(product(0))
    pairs.append(product(1))

    for made in t_z:
        made.wait_recv()
    t_a, t_b, t_far, t_d = {}, {}, {}, []
    for d in (1, 3, 2):
        to = (r, slab(d, 0))
        t_a[d] = (Upper(c, to, y, behind(d, 0)[1]), whole(c, to))

    zs.append(combine(0, pairs[0]))
    zs.append(combine(1, pairs[1]))
    pairs.append(product(2))
    pairs.append(product(3))
    to_axis_b(0)
    zs.append(combine(2, pairs[2]))

    for e in (1, 3, 2):
        for made in t_a[e]:
            made.wait_recv()
        to_axis_b(e)
        if e == 1:
            zs.append(combine(3, pairs[3]))
        if e == 3:
            onward(0)
    for e in (1, 3, 2):
        onward(e)
    for e in (0, 1, 3, 2):
        for made in t_far[e]:
            made.wait_recv()
        to_partner(e, 2)

    def rhs(p):
        parts = []
        for q in range(2):
            k = CHUNKS.index((p, q))
            for made in zs[k]:
                made.wait_recv()
            total = ownf[k, pl.ds(z * 16, 16), :]
            for d in range(1, NZ):
                total = total + zrecv[k, d].astype(F32)
            parts.append(total)
        return jnp.concatenate(parts, axis=1)

    def tile(m, kb, zs_):
        cols = []
        for zz in zs_:
            cols.append(
                jnp.concatenate(
                    [cg[h, cc, zz] if m == 2 else tt[h, cc, zz, m] for cc in range(4 * kb, 4 * kb + 4) for h in range(2)], axis=0
                )
            )
        return jnp.concatenate(cols, axis=1)

    def upper(m, value, q):
        total = None
        for kb in range(q, 4):
            part = jnp.dot(
                value[:, kb * 256:(kb + 1) * 256], tile(m, kb, (2 * q, 2 * q + 1)),
                preferred_element_type=F32,
            )
            total = part if total is None else total + part
        return total

    rhs1 = rhs(1).astype(BF16)
    for made in t_d:
        made.wait_recv()
    second = jnp.concatenate([upper(1, rhs1, q) for q in range(4)], axis=1).astype(BF16)
    cross = jnp.concatenate(
        [
            lax.dot_general(
                second, tile(2, kb, range(8)), (((1,), (1,)), ((), ())), preferred_element_type=F32
            )
            for kb in range(4)
        ],
        axis=1,
    )
    rhs0 = (rhs(0) - cross).astype(BF16)
    strip = jnp.concatenate([upper(0, rhs0, q) for q in range(2)], axis=1).astype(BF16)

    own[4].wait()
    lane = iota((16, 256), 1)
    wanted = core * 128 + z * 16 + iota((16, 256), 0)
    weight = jnp.sum(jnp.where(lane == wanted, occ_ref[...], 0.0), axis=1, keepdims=True)
    sc[0, core, z] = (strip.astype(F32) * (weight * 0.015625)).astype(BF16)

    s_z, s_x, s_y = [], [], []
    for d in (1, 7, 4, 2, 6, 3, 5):
        s_z.append((d, copy(sc.at[0, core, z], sc.at[0, core, z], zdev(d))))

    def spread_out(zz, zin):
        for d in (2, 1, 3):
            s_x.append((d, zin, copy(sc.at[0, core, zz], sc.at[d, core, zz], (r, xcol(d)))))
            s_y.append((3 + d, zin, copy(sc.at[0, core, zz], sc.at[3 + d, core, zz], (r, ycol(d)))))

    spread_out(z, z)

    tail = jnp.concatenate([upper(0, rhs0, q) for q in range(2, 4)], axis=1).astype(BF16)
    first = jnp.concatenate([strip, tail], axis=1)
    for zz in range(NZ):
        po[zz, 0] = first[:, zz * 128:(zz + 1) * 128]
        po[zz, 1] = second[:, zz * 128:(zz + 1) * 128]
    pr[core, z] = po[z]

    for d, made in s_z[:2] + s_z[3:] + s_z[2:3]:
        made.wait_recv()
        zz = lax.rem(z + NZ - d, NZ)
        spread_out(zz, zz)
    s_d = [copy(sc.at[0, core], sc.at[0, core], partner)]

    p_out = []
    for d in range(NZ):
        for other in range(2):
            if d or other:
                dev = zdev(d, other)
                p_out.append(copy(po.at[lax.rem(z + d, NZ)], pr.at[core, z], dev))

    for pair in zip(s_x, s_y):
        for g, zz, made in pair:
            made.wait_recv()
            s_d.append(copy(sc.at[g, core, zz], sc.at[g, core, zz], partner))
    for made in rc_x + rc_y + s_d:
        made.wait_recv()

    def along_y(steps):
        rows = [lax.rem(y + d, SIDE) for d in steps]
        total = 0.0
        for g in range(SIDE):
            block = jnp.concatenate([rca[g, k] if g else view[k, x, 0] for k in rows], axis=0)
            total = total + jnp.dot(block, sc[g].reshape(256, 512), preferred_element_type=F32)
        return total

    def along_x(steps):
        rows = [lax.rem(x + d, SIDE) for d in steps]
        total = 0.0
        for g in range(SIDE):
            block = jnp.concatenate([rcb[g, k] if g else view[y, k, 1] for k in rows], axis=0)
            slot = 3 + g if g else 0
            total = total + jnp.dot(block, sc[slot].reshape(256, 512), preferred_element_type=F32)
        return total

    far = (2, 1, 3)
    pa[...] = along_y(far).astype(BF16).reshape(3, 80, 512)
    r_y = [copy(pa.at[k], ra.at[d], (r, ycol(d))) for k, d in enumerate(far)]
    pb[...] = along_x(far).astype(BF16).reshape(3, 80, 512)
    r_x = [copy(pb.at[k], rb.at[d], (r, xcol(d))) for k, d in enumerate(far)]
    paf[...] = along_y((0,))
    pbf[...] = along_x((0,))

    for made in p_out:
        made.wait_recv()
    for p in range(2):
        states = jnp.concatenate([pr[k, zz, p] for k in range(2) for zz in range(NZ)], axis=0)
        turn[p] = states.astype(F32).T
        panel_ref[p] = turn[p, pl.ds(core * 64, 64), :].astype(BF16)

    for made in r_y:
        made.wait_recv()
    total = paf[...]
    for d in range(1, SIDE):
        total = total + ra[d].astype(F32)
    dens_ref[pl.ds(0, 80), :] = total.astype(BF16)
    for made in r_x:
        made.wait_recv()
    total = pbf[...]
    for d in range(1, SIDE):
        total = total + rb[d].astype(F32)
    dens_ref[pl.ds(80, 80), :] = total.astype(BF16)

    for made in started:
        made.wait_send()


def settle(panel_in, dens_in, panel_out, dens_out, sem):
    moves = [
        pltpu.make_async_copy(panel_in, panel_out, sem.at[0]),
        pltpu.make_async_copy(dens_in, dens_out, sem.at[1]),
    ]
    for move in moves:
        move.start()
    for move in moves:
        move.wait()


def body(y_panels, tri_inverse, coupling, rest_factor, rest_coeffs, occupations):
    rest = rest_coeffs.shape[0]
    vmem = pl.BlockSpec(memory_space=pltpu.VMEM)
    anywhere = pl.BlockSpec(memory_space=pltpu.HBM)
    copies = 300
    shapes = (
        jax.ShapeDtypeStruct((2, 64, 256), BF16),
        jax.ShapeDtypeStruct((160, 512), BF16),
    )
    results = pl.pallas_call(
        kernel,
        out_shape=shapes,
        in_specs=[anywhere] * 6,
        out_specs=(vmem, vmem),
        scratch_shapes=[
            pltpu.VMEM((2, 64, 256), BF16),
            pltpu.VMEM((2, 64, 64), BF16),
            pltpu.VMEM((64, 64), BF16),
            pltpu.VMEM((rest, 256), BF16),
            pltpu.VMEM((1, 256), F32),
            pltpu.VMEM((8, 2 * rest, 128), BF16),
            pltpu.VMEM((2, 256, 2 * rest), BF16),
            pltpu.VMEM((3, 64, 128), BF16),
            pltpu.VMEM((3, 64, 128), BF16),
            pltpu.VMEM((2, 16, NZ, 2, 32, 128), BF16),
            pltpu.VMEM((2, 16, NZ, 32, 128), BF16),
            pltpu.VMEM((4, 128, WIDE), F32),
            pltpu.VMEM((4, 128, WIDE), BF16),
            pltpu.VMEM((4, 128, WIDE), BF16),
            pltpu.VMEM((4, NZ, 16, WIDE), BF16),
            pltpu.VMEM((4, NZ, 16, WIDE), BF16),
            pltpu.VMEM((7, 2, NZ, 16, 512), BF16),
            pltpu.VMEM((SIDE, SIDE, 80, 256), BF16),
            pltpu.VMEM((SIDE, SIDE, 80, 256), BF16),
            pltpu.VMEM((3, 80, 512), BF16),
            pltpu.VMEM((3, 80, 512), BF16),
            pltpu.VMEM((80, 512), F32),
            pltpu.VMEM((80, 512), F32),
            pltpu.VMEM((SIDE, 80, 512), BF16),
            pltpu.VMEM((SIDE, 80, 512), BF16),
            pltpu.VMEM((NZ, 2, 16, 128), BF16),
            pltpu.VMEM((2, NZ, 2, 16, 128), BF16),
            pltpu.VMEM((2, 128, 256), F32),
            pltpu.SemaphoreType.DMA((13,)),
            pltpu.SemaphoreType.DMA((copies,)),
            pltpu.SemaphoreType.DMA((copies,)),
        ],
        compiler_params=pltpu.CompilerParams(
            collective_id=0, has_side_effects=True, vmem_limit_bytes=60 * 1024 * 1024
        ),
    )(y_panels, tri_inverse, coupling, rest_factor, rest_coeffs, occupations.reshape(1, 256))
    return pl.pallas_call(
        settle,
        out_shape=shapes,
        in_specs=[vmem, vmem],
        out_specs=(anywhere, anywhere),
        scratch_shapes=[pltpu.SemaphoreType.DMA((2,))],
        compiler_params=pltpu.CompilerParams(vmem_limit_bytes=60 * 1024 * 1024),
    )(*results)


def solution(mesh):
    return jax.shard_map(
        body,
        mesh=mesh,
        in_specs=(
            P(None, "row", "col"),
            P(None, "row", "col"),
            P("row", "col"),
            P("row", None, None),
            P("row", "col"),
            P("col"),
        ),
        out_specs=(P(None, "row", "col"), P(("row", "col"), None)),
        check_vma=False,
    )
```

```python
import jax
import jax.numpy as jnp
from jax import lax
from jax.experimental import pallas as pl
from jax.experimental.pallas import tpu as pltpu
from jax.sharding import PartitionSpec as P

MESH = pl.DeviceIdType.MESH
BF16 = jnp.bfloat16
F32 = jnp.float32
NZ = 8
SIDE = 4
KB = 256
CHUNKS = ((1, 0), (1, 1), (0, 0), (0, 1))
WIDE = 512


def iota(shape, dim):
    return lax.broadcasted_iota(jnp.int32, shape, dim)


def kernel(
    y_in, tri_in, coup_in, fac_ref, rc_in, occ_in,
    panel_ref, dens_ref,
    y_ref, tri_ref, coup_ref, rc_ref, occ_ref,
    fbuf, rci, tsend, trecv, tt, cg, ownf, psend, precv, zsend, zrecv,
    sc, rca, rcb, pa, pb, paf, pbf, ra, rb, po, pr, turn,
    fsem, send_sem, recv_sem,
):
    r = lax.axis_index("row")
    c = lax.axis_index("col")
    z, core = r // 2, r % 2
    y, x = c // SIDE, c % SIDE
    rest = rc_ref.shape[0]
    count = [0]
    started = []

    def zdev(d, other=0):
        k = core if not other else 1 - core
        return (lax.rem(z + d, NZ) * 2 + k, c)

    def xcol(d):
        return y * SIDE + lax.rem(x + d, SIDE)

    def ycol(d):
        return lax.rem(y + d, SIDE) * SIDE + x

    def copy(src, dst, dev):
        k = count[0]
        count[0] += 1
        made = pltpu.make_async_remote_copy(
            src_ref=src, dst_ref=dst, send_sem=send_sem.at[k], recv_sem=recv_sem.at[k],
            device_id=dev, device_id_type=MESH,
        )
        made.start()
        started.append(made)
        return made

    partner = zdev(0, 1)

    barrier = pltpu.get_barrier_semaphore()
    greeted = [partner]
    for d in range(1, NZ):
        greeted += [zdev(d), zdev(d, 1)]
    for d in range(1, SIDE):
        greeted += [(r, xcol(d)), (r, ycol(d))]
    for dev in greeted:
        pl.semaphore_signal(barrier, inc=1, device_id=dev, device_id_type=MESH)

    own = []
    for k, (src, dst) in enumerate(
        ((tri_in, tri_ref), (coup_in, coup_ref), (rc_in, rc_ref), (y_in, y_ref), (occ_in, occ_ref))
    ):
        own.append(pltpu.make_async_copy(src, dst, fsem.at[8 + k]))
        own[k].start()

    loads = []
    for nb in range(8):
        load = pltpu.make_async_copy(
            fac_ref.reshape(2 * rest, 1024).at[:, pl.ds(nb * 128, 128)], fbuf.at[nb], fsem.at[nb]
        )
        loads.append(load)
    for nb in range(8):
        loads[nb].start()

    own[0].wait()
    own[1].wait()
    for m in range(3):
        block = (coup_ref[...] if m == 2 else tri_ref[m]).astype(F32).T.astype(BF16)
        tsend[m] = jnp.concatenate([block, block], axis=1)

    own[2].wait()
    krow, kcol = iota((KB, 2 * KB), 0), iota((KB, 2 * KB), 1)
    spread = [jnp.where(kcol == 2 * krow + p, -1.0, 0.0).astype(BF16) for p in range(2)]

    def widen(kb, carry):
        turned = rc_ref[pl.ds(pl.multiple_of(kb * KB, KB), KB), :].T
        for p in range(2):
            rci[p, :, pl.ds(pl.multiple_of(kb * 2 * KB, 2 * KB), 2 * KB)] = jnp.dot(
                turned, spread[p], preferred_element_type=F32
            ).astype(BF16)
        return carry

    half = rest // KB // 2
    lax.fori_loop(0, half, widen, 0)

    pl.semaphore_wait(barrier, len(greeted))
    t_pair = copy(tsend, trecv, partner)

    view = rc_ref.reshape(SIDE, SIDE, 2, 80, 256)
    rc_x, rc_y = [], []

    def exchange(d):
        rc_x.append(copy(view.at[:, lax.rem(x + d, SIDE), 0], rca.at[d], (r, xcol(d))))
        rc_y.append(copy(view.at[lax.rem(y + d, SIDE), :, 1], rcb.at[d], (r, ycol(d))))

    for d in (2, 1, 3):
        exchange(d)

    def product(k):
        p, q = CHUNKS[k]
        if p == 1:
            for nb in range(4 * q, 4 * q + 4):
                loads[nb].wait()
        if k == 0:
            own[3].wait()
        turned = y_ref[p].astype(F32).T.astype(BF16)
        here = core == 0

        def columns(n, carry):
            base = q * WIDE + n * 256
            place = (iota((64, 256), 1) + base == r * 64 + iota((64, 256), 0)).astype(F32)
            w = jnp.concatenate([fbuf[4 * q + 2 * n + i] for i in range(2)], axis=1)
            got = jnp.dot(rci[p], w, preferred_element_type=F32) + jnp.dot(
                turned, place.astype(BF16), preferred_element_type=F32
            )
            low, high = got[:128], got[128:]
            lanes = pl.ds(pl.multiple_of(n * 256, 256), 256)
            ownf[k, :, lanes] = jnp.where(here, low, high)
            psend[k, :, lanes] = jnp.where(here, high, low).astype(BF16)
            return carry

        lax.fori_loop(0, 2, columns, 0)
        return copy(psend.at[k], precv.at[k], partner)

    def combine(k, pair):
        pair.wait_recv()
        total = ownf[k] + precv[k].astype(F32)
        ownf[k] = total
        zsend[k] = total.astype(BF16).reshape(NZ, 16, WIDE)
        out = []
        for d in (4, 3, 5, 2, 6, 1, 7):
            out.append(copy(zsend.at[k, lax.rem(z + d, NZ)], zrecv.at[k, d], zdev(d)))
        return out

    pairs, zs = [], []
    is0 = core == 0

    class Upper:
        def __init__(self, cc, to, out, come, sizes=range(SIDE)):
            k = count[0]
            count[0] += 1
            self.out, self.come, self.sizes = out, come, sizes
            self.made = [
                pltpu.make_async_remote_copy(
                    src_ref=tt.at[core, cc, pl.ds(0, 2 * v + 2)],
                    dst_ref=tt.at[core, cc, pl.ds(0, 2 * v + 2)],
                    send_sem=send_sem.at[k], recv_sem=recv_sem.at[k],
                    device_id=to, device_id_type=MESH,
                )
                for v in range(SIDE)
            ]
            for v in sizes:
                pl.when(out == v)(self.made[v].start)
            started.append(self)

        def wait_recv(self):
            for v in self.sizes:
                pl.when(self.come == v)(self.made[v].wait_recv)

        def wait_send(self):
            for v in self.sizes:
                pl.when(self.out == v)(self.made[v].wait_send)

    def whole(cc, to):
        return copy(cg.at[core, cc], cg.at[core, cc], to)

    class Maybe:
        def __init__(self, src, dst, to, out, come):
            k = count[0]
            count[0] += 1
            self.out, self.come = out, come
            self.made = pltpu.make_async_remote_copy(
                src_ref=src, dst_ref=dst, send_sem=send_sem.at[k], recv_sem=recv_sem.at[k],
                device_id=to, device_id_type=MESH,
            )
            pl.when(out)(self.made.start)
            started.append(self)

        def wait_recv(self):
            pl.when(self.come)(self.made.wait_recv)

        def wait_send(self):
            pl.when(self.out)(self.made.wait_send)

    t_pair.wait_recv()
    mine = (iota((32, 128), 1) // 64) == core
    for m in range(3):
        rows = pl.ds(core * 32, 32)
        got = jnp.where(
            mine, tsend[m, rows, :].astype(F32), trecv[m, rows, :].astype(F32)
        ).astype(BF16)
        if m == 2:
            cg[core, c, z] = got
        else:
            tt[core, c, z, m] = got
    t_z = []
    for d in (4, 3, 5, 2, 6, 1, 7):
        t_z.append(copy(cg.at[core, c, z], cg.at[core, c, z], zdev(d)))
        t_z.append(
            Maybe(
                tt.at[core, c, z], tt.at[core, c, z], zdev(d),
                z <= 2 * y + 1, lax.rem(z + NZ - d, NZ) <= 2 * y + 1,
            )
        )

    def moved(a, b):
        dx, dy = jnp.where(is0, a, b), jnp.where(is0, b, a)
        return lax.rem(x + dx, SIDE), lax.rem(y + dy, SIDE)

    def slab(a, b):
        xx, yy = moved(a, b)
        return yy * SIDE + xx

    def behind(e, d):
        back = ((SIDE - e) % SIDE, (SIDE - d) % SIDE)
        return slab(*back), moved(*back)[1], moved(*back[::-1])[1]

    def to_axis_b(e):
        cc, out, _ = behind(e, 0)
        for d in (1, 3):
            to = (r, slab(0, d))
            t_b[e, d] = (Upper(cc, to, out, behind(e, d)[1]), whole(cc, to))
        to_partner(e, 0)

    def onward(e):
        for made in t_b[e, 1] + t_b[e, 3]:
            made.wait_recv()
        far = behind(e, 2)[1]
        (low, low_size, _), (high, high_size, _) = behind(e, 1), behind(e, 3)
        up, down = (r, slab(0, 1)), (r, slab(0, 3))
        last = SIDE - 1
        t_far[e] = (
            Upper(high, down, high_size, far, range(last)),
            Upper(low, up, low_size, far, (last,)),
            Maybe(cg.at[core, low], cg.at[core, low], up, low_size != last, far != last),
            Maybe(cg.at[core, high], cg.at[core, high], down, high_size == last, far == last),
        )
        to_partner(e, 1)
        to_partner(e, 3)

    def to_partner(e, d):
        cc, out, come = behind(e, d)
        t_d.append(Upper(cc, partner, out, come))
        t_d.append(whole(cc, partner))

    lax.fori_loop(half, rest // KB, widen, 0)
    pairs.append(product(0))
    pairs.append(product(1))

    for made in t_z:
        made.wait_recv()
    t_a, t_b, t_far, t_d = {}, {}, {}, []
    for d in (1, 3, 2):
        to = (r, slab(d, 0))
        t_a[d] = (Upper(c, to, y, behind(d, 0)[1]), whole(c, to))

    zs.append(combine(0, pairs[0]))
    zs.append(combine(1, pairs[1]))
    pairs.append(product(2))
    pairs.append(product(3))
    zs.append(combine(2, pairs[2]))

    for e in (1, 3, 2):
        for made in t_a[e]:
            made.wait_recv()
        to_axis_b(e)
        if e == 1:
            to_axis_b(0)
            zs.append(combine(3, pairs[3]))
        if e == 3:
            onward(0)
    for e in (1, 3, 2):
        onward(e)
    for e in (0, 1, 3, 2):
        for made in t_far[e]:
            made.wait_recv()
        to_partner(e, 2)

    def rhs(p):
        parts = []
        for q in range(2):
            k = CHUNKS.index((p, q))
            for made in zs[k]:
                made.wait_recv()
            total = ownf[k, pl.ds(z * 16, 16), :]
            for d in range(1, NZ):
                total = total + zrecv[k, d].astype(F32)
            parts.append(total)
        return jnp.concatenate(parts, axis=1)

    def tile(m, kb, zs_):
        cols = []
        for zz in zs_:
            cols.append(
                jnp.concatenate(
                    [cg[h, cc, zz] if m == 2 else tt[h, cc, zz, m] for cc in range(4 * kb, 4 * kb + 4) for h in range(2)], axis=0
                )
            )
        return jnp.concatenate(cols, axis=1)

    def upper(m, value, q):
        total = None
        for kb in range(q, 4):
            part = jnp.dot(
                value[:, kb * 256:(kb + 1) * 256], tile(m, kb, (2 * q, 2 * q + 1)),
                preferred_element_type=F32,
            )
            total = part if total is None else total + part
        return total

    rhs1 = rhs(1).astype(BF16)
    for made in t_d:
        made.wait_recv()
    second = jnp.concatenate([upper(1, rhs1, q) for q in range(4)], axis=1).astype(BF16)
    cross = jnp.concatenate(
        [
            lax.dot_general(
                second, tile(2, kb, range(8)), (((1,), (1,)), ((), ())), preferred_element_type=F32
            )
            for kb in range(4)
        ],
        axis=1,
    )
    rhs0 = (rhs(0) - cross).astype(BF16)
    strip = jnp.concatenate([upper(0, rhs0, q) for q in range(2)], axis=1).astype(BF16)

    own[4].wait()
    lane = iota((16, 256), 1)
    wanted = core * 128 + z * 16 + iota((16, 256), 0)
    weight = jnp.sum(jnp.where(lane == wanted, occ_ref[...], 0.0), axis=1, keepdims=True)
    sc[0, core, z] = (strip.astype(F32) * (weight * 0.015625)).astype(BF16)

    s_z, s_x, s_y = [], [], []
    for d in (1, 7, 4, 2, 6, 3, 5):
        s_z.append((d, copy(sc.at[0, core, z], sc.at[0, core, z], zdev(d))))

    def spread_out(zz, zin):
        for d in (2, 1, 3):
            s_x.append((d, zin, copy(sc.at[0, core, zz], sc.at[d, core, zz], (r, xcol(d)))))
            s_y.append((3 + d, zin, copy(sc.at[0, core, zz], sc.at[3 + d, core, zz], (r, ycol(d)))))

    spread_out(z, z)

    tail = jnp.concatenate([upper(0, rhs0, q) for q in range(2, 4)], axis=1).astype(BF16)
    first = jnp.concatenate([strip, tail], axis=1)
    for zz in range(NZ):
        po[zz, 0] = first[:, zz * 128:(zz + 1) * 128]
        po[zz, 1] = second[:, zz * 128:(zz + 1) * 128]
    pr[core, z] = po[z]

    for d, made in s_z[:2] + s_z[3:] + s_z[2:3]:
        made.wait_recv()
        zz = lax.rem(z + NZ - d, NZ)
        spread_out(zz, zz)
    s_d = [copy(sc.at[0, core], sc.at[0, core], partner)]

    p_out = []
    for d in range(NZ):
        for other in range(2):
            if d or other:
                dev = zdev(d, other)
                p_out.append(copy(po.at[lax.rem(z + d, NZ)], pr.at[core, z], dev))

    for pair in zip(s_x, s_y):
        for g, zz, made in pair:
            made.wait_recv()
            s_d.append(copy(sc.at[g, core, zz], sc.at[g, core, zz], partner))
    for made in rc_x + rc_y + s_d:
        made.wait_recv()

    def along_y(steps):
        rows = [lax.rem(y + d, SIDE) for d in steps]
        total = 0.0
        for g in range(SIDE):
            block = jnp.concatenate([rca[g, k] if g else view[k, x, 0] for k in rows], axis=0)
            total = total + jnp.dot(block, sc[g].reshape(256, 512), preferred_element_type=F32)
        return total

    def along_x(steps):
        rows = [lax.rem(x + d, SIDE) for d in steps]
        total = 0.0
        for g in range(SIDE):
            block = jnp.concatenate([rcb[g, k] if g else view[y, k, 1] for k in rows], axis=0)
            slot = 3 + g if g else 0
            total = total + jnp.dot(block, sc[slot].reshape(256, 512), preferred_element_type=F32)
        return total

    far = (2, 1, 3)
    pa[...] = along_y(far).astype(BF16).reshape(3, 80, 512)
    r_y = [copy(pa.at[k], ra.at[d], (r, ycol(d))) for k, d in enumerate(far)]
    pb[...] = along_x(far).astype(BF16).reshape(3, 80, 512)
    r_x = [copy(pb.at[k], rb.at[d], (r, xcol(d))) for k, d in enumerate(far)]
    paf[...] = along_y((0,))
    pbf[...] = along_x((0,))

    for made in p_out:
        made.wait_recv()
    for p in range(2):
        states = jnp.concatenate([pr[k, zz, p] for k in range(2) for zz in range(NZ)], axis=0)
        turn[p] = states.astype(F32).T
        panel_ref[p] = turn[p, pl.ds(core * 64, 64), :].astype(BF16)

    for made in r_y:
        made.wait_recv()
    total = paf[...]
    for d in range(1, SIDE):
        total = total + ra[d].astype(F32)
    dens_ref[pl.ds(0, 80), :] = total.astype(BF16)
    for made in r_x:
        made.wait_recv()
    total = pbf[...]
    for d in range(1, SIDE):
        total = total + rb[d].astype(F32)
    dens_ref[pl.ds(80, 80), :] = total.astype(BF16)

    for made in started:
        made.wait_send()


def settle(panel_in, dens_in, panel_out, dens_out, sem):
    moves = [
        pltpu.make_async_copy(panel_in, panel_out, sem.at[0]),
        pltpu.make_async_copy(dens_in, dens_out, sem.at[1]),
    ]
    for move in moves:
        move.start()
    for move in moves:
        move.wait()


def body(y_panels, tri_inverse, coupling, rest_factor, rest_coeffs, occupations):
    rest = rest_coeffs.shape[0]
    vmem = pl.BlockSpec(memory_space=pltpu.VMEM)
    anywhere = pl.BlockSpec(memory_space=pltpu.HBM)
    copies = 300
    shapes = (
        jax.ShapeDtypeStruct((2, 64, 256), BF16),
        jax.ShapeDtypeStruct((160, 512), BF16),
    )
    results = pl.pallas_call(
        kernel,
        out_shape=shapes,
        in_specs=[anywhere] * 6,
        out_specs=(vmem, vmem),
        scratch_shapes=[
            pltpu.VMEM((2, 64, 256), BF16),
            pltpu.VMEM((2, 64, 64), BF16),
            pltpu.VMEM((64, 64), BF16),
            pltpu.VMEM((rest, 256), BF16),
            pltpu.VMEM((1, 256), F32),
            pltpu.VMEM((8, 2 * rest, 128), BF16),
            pltpu.VMEM((2, 256, 2 * rest), BF16),
            pltpu.VMEM((3, 64, 128), BF16),
            pltpu.VMEM((3, 64, 128), BF16),
            pltpu.VMEM((2, 16, NZ, 2, 32, 128), BF16),
            pltpu.VMEM((2, 16, NZ, 32, 128), BF16),
            pltpu.VMEM((4, 128, WIDE), F32),
            pltpu.VMEM((4, 128, WIDE), BF16),
            pltpu.VMEM((4, 128, WIDE), BF16),
            pltpu.VMEM((4, NZ, 16, WIDE), BF16),
            pltpu.VMEM((4, NZ, 16, WIDE), BF16),
            pltpu.VMEM((7, 2, NZ, 16, 512), BF16),
            pltpu.VMEM((SIDE, SIDE, 80, 256), BF16),
            pltpu.VMEM((SIDE, SIDE, 80, 256), BF16),
            pltpu.VMEM((3, 80, 512), BF16),
            pltpu.VMEM((3, 80, 512), BF16),
            pltpu.VMEM((80, 512), F32),
            pltpu.VMEM((80, 512), F32),
            pltpu.VMEM((SIDE, 80, 512), BF16),
            pltpu.VMEM((SIDE, 80, 512), BF16),
            pltpu.VMEM((NZ, 2, 16, 128), BF16),
            pltpu.VMEM((2, NZ, 2, 16, 128), BF16),
            pltpu.VMEM((2, 128, 256), F32),
            pltpu.SemaphoreType.DMA((13,)),
            pltpu.SemaphoreType.DMA((copies,)),
            pltpu.SemaphoreType.DMA((copies,)),
        ],
        compiler_params=pltpu.CompilerParams(
            collective_id=0, has_side_effects=True, vmem_limit_bytes=60 * 1024 * 1024
        ),
    )(y_panels, tri_inverse, coupling, rest_factor, rest_coeffs, occupations.reshape(1, 256))
    return pl.pallas_call(
        settle,
        out_shape=shapes,
        in_specs=[vmem, vmem],
        out_specs=(anywhere, anywhere),
        scratch_shapes=[pltpu.SemaphoreType.DMA((2,))],
        compiler_params=pltpu.CompilerParams(vmem_limit_bytes=60 * 1024 * 1024),
    )(*results)


def solution(mesh):
    return jax.shard_map(
        body,
        mesh=mesh,
        in_specs=(
            P(None, "row", "col"),
            P(None, "row", "col"),
            P("row", "col"),
            P("row", None, None),
            P("row", "col"),
            P("col"),
        ),
        out_specs=(P(None, "row", "col"), P(("row", "col"), None)),
        check_vma=False,
    )
```
